256 devices in a mesh: dp: 64 (over z, y, core), tp: 4 (over x).
Axes of the slice: x: 4, y: 4, z: 8, core: 2. Of those that a mesh axis runs over, the one named last changes fastest.
Arguments:
- partial_up: bfloat16 [64, 1024, 4096], P('dp', None, 'tp'), may hold values from -8 to 8
- partial_down: bfloat16 [64, 4096, 1024], P('dp', 'tp'), may hold values from -8 to 8
- partial_norm: bfloat16 [64, 1024], P('dp'), may hold values from -16 to 16
- master_up: float32 [1024, 4096], P('dp', 'tp'), may hold values from -0.5 to 0.5
- master_down: float32 [4096, 1024], P('tp', 'dp'), may hold values from -0.25 to 0.25
- master_norm: float32 [1024], P('dp'), may hold values from 0.25 to 1.75
- memory_up: float32 [1024, 4096], P('dp', 'tp'), may hold values from 0.0001953125 to 0.001953125
- memory_down: float32 [4096, 1024], P('tp', 'dp'), may hold values from 4.8828126e-05 to 0.00048828125
- memory_norm: float32 [1024], P('dp'), may hold values from 0.05 to 0.8
Outputs:
- compute_up: bfloat16 [1024, 4096], P(None, 'tp')
- compute_down: bfloat16 [4096, 1024], P('tp')
- compute_norm: bfloat16 [1024], replicated
- stepped_up: float32 [1024, 4096], P('dp', 'tp')
- stepped_down: float32 [4096, 1024], P('tp', 'dp')
- stepped_norm: float32 [1024], P('dp')
- state_new_up: float32 [1024, 4096], P('dp', 'tp')
- state_new_down: float32 [4096, 1024], P('tp', 'dp')
- state_new_norm: float32 [1024], P('dp')
The draws below stay inside these ranges and needn't reach their ends.
All inputs are finite; a program needn't handle non-finite values.
Results may differ from the reference program's by a relative error of at most 0.001.
Values may be sent and summed in bfloat16 or wider, within the bound.
A program may use at most 64 MiB of HBM per device.

```python
import jax
import jax.numpy as jnp
from jax import lax

WIDTH = 1024
INNER = 4096
REPLICAS = 64


def raised(values, own_key, source, target, shards_of, factor):
    def block_of(axis_at):
        return (jnp.arange(values.shape[axis_at]) // (values.shape[axis_at] // shards_of)).reshape((-1,) + (1,) * (values.ndim - 1 - axis_at))

    near = jax.random.permutation(own_key, shards_of)[block_of(target)]
    far = (block_of(target) + shards_of // 2) % shards_of
    return jnp.where((block_of(source) == near) | (block_of(source) == far), factor * values, values)


def block_levels(rng, extent, cuts, low, largest):
    def one(dim, shards_of):
        steps = jax.random.uniform(jax.random.fold_in(jax.random.fold_in(rng, 6), dim), (shards_of,), jnp.float32, low / len(cuts), largest / len(cuts))
        return jnp.repeat(jnp.exp(steps), extent[dim] // shards_of).reshape((-1,) + (1,) * (len(extent) - dim - 1))

    factor_of = one(*cuts[0])
    for cut in cuts[1:]:
        factor_of = factor_of * one(*cut)
    return factor_of


def noise_with(key, extent, width, limit, shards, heavy, kind=jnp.bfloat16):
    array = width * jax.random.normal(key, extent, jnp.float32)
    if shards:
        array = array * block_levels(key, extent, shards, -0.22, 0.18)
    return jnp.clip(raised(array, jax.random.fold_in(key, 3), *heavy), -limit, limit).astype(kind)


def setup_inputs(seed: int = 0) -> dict:
    streams_of = jax.random.split(jax.random.key(seed), 10)
    partial_up = noise_with(streams_of[0], (REPLICAS, WIDTH, INNER), 0.5, 8.0, ((0, 64), (2, 4)), (0, 1, 64, 4.0))
    partial_down = noise_with(streams_of[1], (REPLICAS, INNER, WIDTH), 0.5, 8.0, ((0, 64), (1, 4)), (0, 2, 64, 4.0))
    partial_norm = noise_with(streams_of[2], (REPLICAS, WIDTH), 1.0, 16.0, ((0, 64),), (0, 1, 64, 4.0))
    master_up = noise_with(streams_of[3], (WIDTH, INNER), WIDTH ** -0.5, 0.5, ((0, 64), (1, 4)), (1, 0, 64, 4.0), jnp.float32)
    master_down = noise_with(streams_of[4], (INNER, WIDTH), INNER ** -0.5, 0.25, ((0, 4), (1, 64)), (0, 1, 64, 4.0), jnp.float32)
    master_norm = jnp.clip(1.0 + 0.15 * jax.random.normal(streams_of[5], (WIDTH,), jnp.float32), 0.25, 1.75)
    memory_up = jnp.clip(0.0001953125 + 0.0017578125 * jax.random.uniform(streams_of[6], (WIDTH, INNER), jnp.float32) ** block_levels(streams_of[6], (WIDTH, INNER), ((0, 64), (1, 4)), -0.2, 0.2), 0.0001953125, 0.001953125)
    memory_down = jnp.clip(4.882812572759576e-05 + 0.0004394531 * jax.random.uniform(streams_of[7], (INNER, WIDTH), jnp.float32) ** block_levels(streams_of[7], (INNER, WIDTH), ((0, 4), (1, 64)), -0.2, 0.2), 4.882812572759576e-05, 0.00048828125)
    memory_norm = jnp.clip(0.05 + 0.75 * jax.random.uniform(streams_of[8], (WIDTH,), jnp.float32) ** block_levels(streams_of[8], (WIDTH,), ((0, 64),), -0.2, 0.2), 0.05, 0.8)
    return {"partial_up": partial_up, "partial_down": partial_down, "partial_norm": partial_norm, "master_up": master_up, "master_down": master_down, "master_norm": master_norm, "memory_up": memory_up, "memory_down": memory_down, "memory_norm": memory_norm}


learn_rate = 0.025
hold_rate = 0.8

def reference(partial_up, partial_down, partial_norm, master_up, master_down, master_norm, memory_up, memory_down, memory_norm):
    mean_up = lax.optimization_barrier(jnp.sum(partial_up.astype(jnp.float32), axis=0)) * REPLICAS ** (-0.5)
    mean_down = lax.optimization_barrier(jnp.sum(partial_down.astype(jnp.float32), axis=0)) * REPLICAS ** (-0.5)
    mean_norm = lax.optimization_barrier(jnp.sum(partial_norm.astype(jnp.float32), axis=0)) * REPLICAS ** (-0.5)
    ratio_up = jnp.sqrt(lax.optimization_barrier(jnp.sum(master_up * master_up, axis=1, keepdims=True))) * lax.rsqrt(lax.optimization_barrier(jnp.sum(mean_up * mean_up, axis=1, keepdims=True)) + 1e-06)
    mean_up = mean_up * ratio_up
    ratio_down = jnp.sqrt(lax.optimization_barrier(jnp.sum(master_down * master_down, axis=0, keepdims=True))) * lax.rsqrt(lax.optimization_barrier(jnp.sum(mean_down * mean_down, axis=0, keepdims=True)) + 1e-06)
    mean_down = mean_down * ratio_down
    state_new_up = hold_rate * memory_up + (1.0 - hold_rate) * mean_up * mean_up
    stepped_up = master_up - learn_rate * mean_up * lax.rsqrt(state_new_up + 1e-06)
    state_new_down = hold_rate * memory_down + (1.0 - hold_rate) * mean_down * mean_down
    stepped_down = master_down - learn_rate * mean_down * lax.rsqrt(state_new_down + 1e-06)
    state_new_norm = hold_rate * memory_norm + (1.0 - hold_rate) * mean_norm * mean_norm
    stepped_norm = master_norm - learn_rate * mean_norm * lax.rsqrt(state_new_norm + 1e-06)
    compute_up = stepped_up.astype(jnp.bfloat16)
    compute_down = stepped_down.astype(jnp.bfloat16)
    compute_norm = stepped_norm.astype(jnp.bfloat16)
    return (compute_up, compute_down, compute_norm, stepped_up, stepped_down, stepped_norm, state_new_up, state_new_down, state_new_norm)
```

```python
import functools

import jax
import jax.numpy as jnp
from jax import lax
from jax.experimental import pallas as pl
from jax.experimental.pallas import tpu as pltpu
from jax.sharding import Mesh
from jax.sharding import PartitionSpec as P

DP = ("dp_0", "dp_1", "dp_2")
NZ, NY, NC, NX = 8, 4, 2, 4
MESH = pl.DeviceIdType.MESH
F32, BF16 = jnp.float32, jnp.bfloat16

learn_rate = 0.025
hold_rate = 0.8


def updated(master, memory, mean):
    state = hold_rate * memory + (1.0 - hold_rate) * mean * mean
    return master - learn_rate * mean * lax.rsqrt(state + 1e-06), state


def slots_of(n):
    out = [(n // 2, 0)]
    for k in range(n // 2 - 1, 0, -1):
        out += [(k, 1), (k, 0)]
    return out


def kernel(
    small, pu, pd, mu, md, vu, vd,
    out_u, out_d, nout, su, sd, qu, qd,
    own_u, pr_u, own_d, pr_d, ds, dr, us, ur, sum_u, zs, zr, gs, gr, tps, tpr, gds, gd, sms, smr,
    loc_u, loc_d, s0_send, s0u_recv, s0d_recv, d_send, d_recv, u_send, u_recv, z_send, z_recv,
    g_send, g_recv, t_send, t_recv, sm_send, sm_recv,
    agz_send, agz_recv, agy_send, agy_recv, agd_send, agd_recv, gd_send, gd_recv, pair_send, pair_recv,
):
    z, y, c, x = (lax.axis_index(a) for a in ("dp_0", "dp_1", "dp_2", "tp"))
    o = 1 - c
    zo = lambda k: lax.rem(z + k + NZ, NZ)
    yo = lambda k: lax.rem(y + k + NY, NY)

    def rcopy(src, dst, ssem, rsem, **dev):
        cp = pltpu.make_async_remote_copy(
            src_ref=src, dst_ref=dst, send_sem=ssem, recv_sem=rsem, device_id=dev, device_id_type=MESH
        )
        return cp

    def started(*args, **dev):
        rcopy(*args, **dev).start()

    def arrived(dst, rsem):
        pltpu.make_async_copy(dst, dst, rsem).wait()

    zorder = (4, 3, -3, 2, -2, 1, -1, 0)
    yorder = (2, 1, -1, 0)
    col = lambda zt: pl.ds(pl.multiple_of(zt * 128, 128), 128)
    for i, k in enumerate(zorder):
        pltpu.make_async_copy(pd.at[c, :, col(zo(k))], own_d.at[zo(k)], loc_d.at[i]).start()
    for i, k in enumerate(yorder):
        pltpu.make_async_copy(pu.at[:, yo(k), c], own_u.at[:, yo(k)], loc_u.at[i]).start()

    barrier = pltpu.get_barrier_semaphore()
    peers = [{"dp_0": zo(k)} for k in range(1, NZ)]
    peers += [{"dp_1": yo(dy), "dp_2": lax.rem(c + dc, NC)} for dy in range(NY) for dc in range(NC) if dy or dc]
    peers += [{"tp": lax.rem(x + k, NX)} for k in range(1, NX)]
    for dev in peers:
        pl.semaphore_signal(barrier, inc=1, device_id=dev, device_id_type=MESH)
    pl.semaphore_wait(barrier, len(peers))

    for i in range(8):
        zt = zo(zorder[i])
        started(pd.at[o, :, col(zt)], pr_d.at[zt], s0_send.at[0], s0d_recv.at[i], dp_2=o)
        if i % 2 == 0:
            yt = yo(yorder[i // 2])
            started(pu.at[:, yt, o], pr_u.at[:, yt], s0_send.at[1], s0u_recv.at[i // 2], dp_2=o)
    started(small, smr.at[0], sm_send.at[0], sm_recv.at[0], dp_2=o)

    have = set()

    def need_d(k):
        if ("d", k) not in have:
            have.add(("d", k))
            i = zorder.index(k)
            pltpu.make_async_copy(pd.at[c, :, col(zo(k))], own_d.at[zo(k)], loc_d.at[i]).wait()
            arrived(pr_d.at[zo(k)], s0d_recv.at[i])

    def need_u(k):
        if ("u", k) not in have:
            have.add(("u", k))
            i = yorder.index(k)
            pltpu.make_async_copy(pu.at[:, yo(k), c], own_u.at[:, yo(k)], loc_u.at[i]).wait()
            arrived(pr_u.at[:, yo(k)], s0u_recv.at[i])

    zslots, yslots = slots_of(NZ), slots_of(NY)

    def half_of(direction, h):
        return h if direction == 0 else 1 - h

    def sign(direction):
        return 1 if direction == 0 else -1

    def d_slot(direction, i):
        k, h = zslots[i]
        k = k * sign(direction)
        kk = 4 if k == -4 else k
        need_d(kk)
        rows = pl.ds(half_of(direction, h) * 256, 256)
        val = own_d[zo(kk), rows].astype(F32) + pr_d[zo(kk), rows].astype(F32)
        if i >= 2:
            arrived(dr.at[direction, i - 2], d_recv.at[direction, i - 2])
            val = val + dr[direction, i - 2]
        ds[direction, i] = val
        started(
            ds.at[direction, i], dr.at[direction, i], d_send.at[direction], d_recv.at[direction, i],
            dp_0=zo(sign(direction)),
        )

    def u_slot(direction, i):
        k, h = yslots[i]
        k = k * sign(direction)
        kk = 2 if k == -2 else k
        need_u(kk)
        part = pl.ds(half_of(direction, h) * 4, 4)
        val = own_u[part, yo(kk)].astype(F32) + pr_u[part, yo(kk)].astype(F32)
        if i >= 2:
            arrived(ur.at[direction, i - 2], u_recv.at[direction, i - 2])
            val = val + ur[direction, i - 2]
        us[direction, i] = val
        started(
            us.at[direction, i], ur.at[direction, i], u_send.at[direction], u_recv.at[direction, i],
            dp_1=yo(sign(direction)),
        )

    def z_slot(direction, i):
        k, h = zslots[i]
        k = k * sign(direction)
        rows = pl.ds(half_of(direction, h) * 8, 8)
        val = sum_u[zo(k), rows]
        if i >= 2:
            arrived(zr.at[direction, i - 2], z_recv.at[direction, i - 2])
            val = val + zr[direction, i - 2]
        zs[direction, i] = val
        started(
            zs.at[direction, i], zr.at[direction, i], z_send.at[direction], z_recv.at[direction, i],
            dp_0=zo(sign(direction)),
        )

    for i in (0, 1):
        for direction in (0, 1):
            d_slot(direction, i)
        for direction in (0, 1):
            u_slot(direction, i)

    arrived(smr.at[0], sm_recv.at[0])
    sms[0] = small[...] + smr[0]
    for dy in range(1, NY):
        started(sms.at[0], smr.at[dy], sm_send.at[1], sm_recv.at[dy], dp_1=yo(dy))

    for direction in (0, 1):
        d_slot(direction, 2)
    for direction in (0, 1):
        d_slot(direction, 3)
    for direction in (0, 1):
        u_slot(direction, 2)

    total = sms[0]
    for dy in range(1, NY):
        arrived(smr.at[dy], sm_recv.at[dy])
        total = total + smr[dy]
    sms[1] = total
    for k in range(1, NZ):
        started(sms.at[1], smr.at[3 + k], sm_send.at[2], sm_recv.at[3 + k], dp_0=zo(k))

    for i in (4, 5, 6):
        for direction in (0, 1):
            d_slot(direction, i)

    total = sms[1]
    for k in range(1, NZ):
        arrived(smr.at[3 + k], sm_recv.at[3 + k])
        total = total + smr[3 + k]
    stepped, state = updated(total[8:16], total[16:24], total[0:8] * 0.125)
    nout[0:8] = stepped
    nout[8:16] = state

    need_u(0)
    for h in (0, 1):
        part = pl.ds(4 * h, 4)
        val = own_u[part, y].astype(F32) + pr_u[part, y].astype(F32)
        for direction in (0, 1):
            i = 2 if half_of(direction, 0) == h else 1
            arrived(ur.at[direction, i], u_recv.at[direction, i])
            val = val + ur[direction, i]
        sum_u[part] = val
    for i in (0, 1):
        for direction in (0, 1):
            z_slot(direction, i)

    need_d(0)
    for h in (0, 1):
        rows = pl.ds(256 * h, 256)
        val = own_d[z, rows].astype(F32) + pr_d[z, rows].astype(F32)
        for direction in (0, 1):
            i = 6 if half_of(direction, 0) == h else 5
            arrived(dr.at[direction, i], d_recv.at[direction, i])
            val = val + dr[direction, i]
        for b in (0, 1):
            gs[:, :, pl.ds(256 * h + 128 * b, 128)] = val[128 * b : 128 * b + 128].T.reshape(NY * NC, 16, 128)
    for dy in range(NY):
        for dc in range(NC):
            if dy or dc:
                yt, ct = yo(dy), lax.rem(c + dc, NC)
                started(
                    gs.at[yt * NC + ct], gr.at[c, dy], g_send.at[0], g_recv.at[dy, dc], dp_1=yt, dp_2=ct
                )
    gr[c, 0] = gs[y * NC + c]

    for i in (2, 3, 4, 5, 6):
        for direction in (0, 1):
            z_slot(direction, i)

    lane = lax.broadcasted_iota(jnp.int32, (16, 128), 1)

    def tp_send(which, mean, master):
        own = jnp.sum(master * master, axis=1, keepdims=True)
        slope = jnp.sum(mean * mean, axis=1, keepdims=True)
        tps[which] = jnp.where(lane < 64, own, slope)
        for k in range(1, NX):
            started(
                tps.at[which], tpr.at[which, k - 1], t_send.at[which], t_recv.at[which, k - 1],
                tp=lax.rem(x + k, NX),
            )

    def tp_total(which):
        val = tps[which]
        for k in range(1, NX):
            arrived(tpr.at[which, k - 1], t_recv.at[which, k - 1])
            val = val + tpr[which, k - 1]
        return jnp.sqrt(val[:, 0:1]) * lax.rsqrt(val[:, 64:65] + 1e-06)

    for dy in range(NY):
        for dc in range(NC):
            if dy or dc:
                cs = lax.rem(c + dc, NC)
                arrived(gr.at[cs, dy], g_recv.at[dy, dc])
    for h in (0, 1):
        sd[:, pl.ds(512 * h, 512)] = (gr[h, 0] + gr[h, 1] + gr[h, 2] + gr[h, 3]) * 0.125
    tp_send(1, sd[...], md[...])

    for h in (0, 1):
        rows = pl.ds(8 * h, 8)
        val = sum_u[z, rows]
        for direction in (0, 1):
            i = 6 if half_of(direction, 0) == h else 5
            arrived(zr.at[direction, i], z_recv.at[direction, i])
            val = val + zr[direction, i]
        su[rows] = val * 0.125
    tp_send(0, su[...], mu[...])

    stepped, state = updated(md[...], vd[...], sd[...] * tp_total(1))
    sd[...] = stepped
    qd[...] = state
    turned = stepped.astype(BF16)
    gds[0] = turned[:, :512]
    gds[1] = turned[:, 512:]
    for dy in range(NY):
        for dc in range(NC):
            if dy or dc:
                yt, ct = yo(dy), lax.rem(c + dc, NC)
                started(gds.at[ct], gd.at[y, c], gd_send.at[0], gd_recv.at[dy, dc], dp_1=yt, dp_2=ct)
    gd[y, c] = gds[c]

    stepped, state = updated(mu[...], vu[...], su[...] * tp_total(0))
    su[...] = stepped
    qu[...] = state
    out_u[z, y, c] = stepped.astype(BF16)

    lanes = lambda h: pl.ds(512 * h, 512)

    def to_partner_u(zt, yt):
        piece = out_u.at[zt, yt, c]
        started(piece, piece, pair_send.at[0], pair_recv.at[0], dp_2=o)

    def to_y(kz):
        for direction in (0, 1):
            piece = out_u.at[zo(kz), y, c]
            started(
                piece, piece, agy_send.at[direction], agy_recv.at[direction, 0, kz % NZ], dp_1=yo(sign(direction))
            )
        to_partner_u(zo(kz), y)

    def to_z(direction, k):
        s = sign(direction)
        piece = out_u.at[zo(-s * k), y, c]
        if k == 3:
            piece = piece.at[:, lanes(half_of(direction, 0))]
        started(piece, piece, agz_send.at[direction], agz_recv.at[direction, k], dp_0=zo(s))

    def z_came(direction, k):
        piece = out_u.at[zo(-sign(direction) * k), y, c]
        if k == 4:
            piece = piece.at[:, lanes(half_of(direction, 0))]
        arrived(piece, agz_recv.at[direction, k - 1])

    def y_came(kz):
        for direction in (0, 1):
            s = sign(direction)
            piece = out_u.at[zo(kz), yo(-s), c]
            arrived(piece, agy_recv.at[direction, 0, kz % NZ])
            half = piece.at[:, lanes(direction)]
            started(half, half, agy_send.at[direction], agy_recv.at[direction, 1, kz % NZ], dp_1=yo(s))
            to_partner_u(zo(kz), yo(-s))

    def y_far(kz):
        for direction in (0, 1):
            half = out_u.at[zo(kz), yo(2), c].at[:, lanes(direction)]
            arrived(half, agy_recv.at[direction, 1, kz % NZ])
        to_partner_u(zo(kz), yo(2))

    def d_block(kz, h):
        return out_d.at[pl.ds(pl.multiple_of(c * 512 + h * 256, 256), 256), col(zo(kz))]

    def to_dz(direction, k, h):
        block = d_block(-sign(direction) * k, h)
        started(block, block, agd_send.at[direction], agd_recv.at[direction, k, h], dp_0=zo(sign(direction)))

    def to_partner_d(kz, h):
        block = d_block(kz, h)
        started(block, block, pair_send.at[1], pair_recv.at[1], dp_2=o)

    def turn():
        for dy in range(NY):
            for dc in range(NC):
                if dy or dc:
                    arrived(gd.at[yo(-dy), lax.rem(c + dc, NC)], gd_recv.at[dy, dc])
        for b in range(4):
            block = gd[:, :, :, 128 * b : 128 * b + 128].reshape(128, 128).astype(F32)
            out_d[pl.ds(pl.multiple_of(c * 512 + b * 128, 128), 128), col(z)] = block.T.astype(BF16)
        for h in (0, 1):
            for direction in (0, 1):
                to_dz(direction, 0, half_of(direction, h))
        for h in (0, 1):
            to_partner_d(0, h)

    def d_came(k, h):
        for direction in (0, 1):
            hh = half_of(direction, h)
            if k == 4 and h == 1:
                continue
            arrived(d_block(-sign(direction) * k, hh), agd_recv.at[direction, k - 1, hh])
            if k < 3 or (k == 3 and h == 0):
                to_dz(direction, k, hh)
            to_partner_d(-sign(direction) * k, hh)

    def first_u():
        for direction in (0, 1):
            to_z(direction, 0)
        to_y(0)

    def u_came(k):
        for direction in (0, 1):
            z_came(direction, k)
            if k < 4:
                to_z(direction, k)
        if k < 4:
            for direction in (0, 1):
                to_y(-sign(direction) * k)
        else:
            to_y(4)

    first_u()
    turn()
    u_came(1)
    y_came(0)
    d_came(1, 0)
    u_came(2)
    for kz in (-1, 1):
        y_came(kz)
    y_far(0)
    d_came(1, 1)
    u_came(3)
    for kz in (-2, 2):
        y_came(kz)
    for kz in (-1, 1):
        y_far(kz)
    d_came(2, 0)
    u_came(4)
    for kz in (-3, 3):
        y_came(kz)
    d_came(2, 1)
    for kz in (-2, 2):
        y_far(kz)
    y_came(4)
    d_came(3, 0)
    for kz in (-3, 3):
        y_far(kz)
    d_came(3, 1)
    y_far(4)
    d_came(4, 0)

    for yt in range(NY):
        pass
    arrived(out_u.at[:, :, o], pair_recv.at[0])
    arrived(out_d.at[pl.ds(pl.multiple_of(o * 512, 512), 512)], pair_recv.at[1])

    def left(ref, sem):
        pltpu.make_async_copy(ref, ref, sem).wait()

    left(pr_d, s0_send.at[0])
    left(pr_u, s0_send.at[1])
    left(smr.at[0], sm_send.at[0])
    left(smr.at[pl.ds(0, 3)], sm_send.at[1])
    left(smr.at[pl.ds(0, 7)], sm_send.at[2])
    left(gs.at[pl.ds(0, 7)], g_send.at[0])
    left(own_d.at[0, pl.ds(0, 448)], gd_send.at[0])
    left(out_u.at[:, :, c], pair_send.at[0])
    left(out_d.at[pl.ds(pl.multiple_of(c * 512, 512), 512)], pair_send.at[1])
    for direction in (0, 1):
        left(ds.at[direction], d_send.at[direction])
        left(us.at[direction], u_send.at[direction])
        left(zs.at[direction], z_send.at[direction])
        left(tpr.at[direction], t_send.at[direction])
        left(own_d.at[0, pl.ds(0, 448)], agz_send.at[direction])
        left(own_d.at[pl.ds(0, 3)], agy_send.at[direction])
        left(own_d.at[pl.ds(0, 7), pl.ds(0, 256)], agd_send.at[direction])


def local(pu, pd, pn, mu, md, mn, vu, vd, vn):
    place = lax.axis_index(DP)
    mine = (jnp.arange(1024) // 16 == place).reshape(8, 128)
    placed = lambda v: jnp.where(mine, jnp.tile(v, 64).reshape(8, 128), 0.0)
    small = jnp.concatenate([pn.reshape(8, 128).astype(F32), placed(mn), placed(vn)], axis=0)

    vm = pl.BlockSpec(memory_space=pltpu.VMEM)
    hbm = pl.BlockSpec(memory_space=pl.ANY)
    sds = jax.ShapeDtypeStruct
    dma = pltpu.SemaphoreType.DMA
    half = sds((16, 1024), F32)
    out = pl.pallas_call(
        kernel,
        out_shape=(
            sds((NZ, NY, NC, 16, 1024), BF16), sds((1024, 1024), BF16), sds((16, 128), F32), half, half, half, half,
        ),
        in_specs=[vm, hbm, hbm, vm, vm, vm, vm],
        out_specs=(vm,) * 7,
        scratch_shapes=[
            pltpu.VMEM((NZ, NY, 16, 1024), BF16),
            pltpu.VMEM((NZ, NY, 16, 1024), BF16),
            pltpu.VMEM((NZ, 512, 128), BF16),
            pltpu.VMEM((NZ, 512, 128), BF16),
            pltpu.VMEM((2, 7, 256, 128), F32),
            pltpu.VMEM((2, 7, 256, 128), F32),
            pltpu.VMEM((2, 3, 4, 16, 1024), F32),
            pltpu.VMEM((2, 3, 4, 16, 1024), F32),
            pltpu.VMEM((NZ, 16, 1024), F32),
            pltpu.VMEM((2, 7, 8, 1024), F32),
            pltpu.VMEM((2, 7, 8, 1024), F32),
            pltpu.VMEM((8, 16, 512), F32),
            pltpu.VMEM((2, 4, 16, 512), F32),
            pltpu.VMEM((2, 16, 128), F32),
            pltpu.VMEM((2, 3, 16, 128), F32),
            pltpu.VMEM((2, 16, 512), BF16),
            pltpu.VMEM((4, 2, 16, 512), BF16),
            pltpu.VMEM((2, 24, 128), F32),
            pltpu.VMEM((11, 24, 128), F32),
            dma((4,)), dma((8,)), dma((2,)), dma((4,)), dma((8,)),
            dma((2,)), dma((2, 7)), dma((2,)), dma((2, 3)), dma((2,)), dma((2, 7)),
            dma((1,)), dma((4, 2)), dma((2,)), dma((2, 3)), dma((3,)), dma((11,)),
            dma((2,)), dma((2, 4)), dma((2,)), dma((2, 2, 8)), dma((2,)), dma((2, 4, 2)),
            dma((1,)), dma((4, 2)), dma((2,)), dma((2,)),
        ],
        compiler_params=pltpu.CompilerParams(collective_id=0, has_side_effects=True),
        name="update",
    )(small, pu.reshape(NZ, NY, NC, 16, 1024), pd.reshape(2, 512, 1024), mu, md.T, vu, vd.T)
    out_u, out_d, nout, su, sd, qu, qd = out
    own = lambda t: lax.dynamic_slice_in_dim(t.reshape(1024), place * 16, 16)
    return (
        out_u.reshape(1024, 1024), out_d, nout[0:8].reshape(1024).astype(BF16),
        su, sd.T, own(nout[0:8]), qu, qd.T, own(nout[8:16]),
    )


def solution(mesh):
    finer = Mesh(mesh.devices.reshape(NZ, NY, NC, mesh.shape["tp"]), (*DP, "tp"))
    return jax.shard_map(
        local,
        mesh=finer,
        in_specs=(
            P(DP, None, "tp"), P(DP, "tp", None), P(DP, None),
            P(DP, "tp"), P("tp", DP), P(DP),
            P(DP, "tp"), P("tp", DP), P(DP),
        ),
        out_specs=(
            P(None, "tp"), P("tp", None), P(),
            P(DP, "tp"), P("tp", DP), P(DP),
            P(DP, "tp"), P("tp", DP), P(DP),
        ),
        check_vma=False,
    )
```

```python
import functools

import jax
import jax.numpy as jnp
from jax import lax
from jax.experimental import pallas as pl
from jax.experimental.pallas import tpu as pltpu
from jax.sharding import Mesh
from jax.sharding import PartitionSpec as P

DP = ("dp_0", "dp_1", "dp_2")
NZ, NY, NC, NX = 8, 4, 2, 4
MESH = pl.DeviceIdType.MESH
F32, BF16 = jnp.float32, jnp.bfloat16

learn_rate = 0.025
hold_rate = 0.8

VMEM_LIMIT = int(49 * 2**20)


def updated(master, memory, mean):
    state = hold_rate * memory + (1.0 - hold_rate) * mean * mean
    return master - learn_rate * mean * lax.rsqrt(state + 1e-06), state


def slots_of(n):
    out = [(n // 2, 0)]
    for k in range(n // 2 - 1, 0, -1):
        out += [(k, 1), (k, 0)]
    return out


def kernel(
    own, pu_in, pd_in,
    out_u, out_d, state_out, nout,
    pu, pd, pr_u, pr_d, ds, dr, us, ur, sum_u, zs, zr, gs, gr, tps, tpr, gds, gd, sms, smr, rolled, su, sd,
    loc, s0_send, s0u_recv, s0d_recv, d_send, d_recv, u_send, u_recv, z_send, z_recv,
    g_send, g_recv, t_send, t_recv, sm_send, sm_recv,
    agz_send, agz_recv, agy_send, agy_recv, agd_send, agd_recv, gd_send, gd_recv, pair_send, pair_recv,
):
    z, y, c, x = (lax.axis_index(a) for a in ("dp_0", "dp_1", "dp_2", "tp"))
    o = 1 - c
    zo = lambda k: lax.rem(z + k + NZ, NZ)
    yo = lambda k: lax.rem(y + k + NY, NY)

    def rcopy(src, dst, ssem, rsem, **dev):
        cp = pltpu.make_async_remote_copy(
            src_ref=src, dst_ref=dst, send_sem=ssem, recv_sem=rsem, device_id=dev, device_id_type=MESH
        )
        return cp

    def started(*args, **dev):
        rcopy(*args, **dev).start()

    def arrived(dst, rsem):
        pltpu.make_async_copy(dst, dst, rsem).wait()

    zorder = (4, 3, -3, 2, -2, 1, -1, 0)
    yorder = (2, 1, -1, 0)
    col = lambda zt: pl.ds(pl.multiple_of(zt * 128, 128), 128)

    pltpu.make_async_copy(pd_in, pd, loc.at[0]).start()
    pltpu.make_async_copy(pu_in, pu, loc.at[1]).start()
    mu, md, vu, vd = (own.at[pl.ds(16 * i, 16)] for i in range(4))

    spread = lax.rem(16 * (y * NC + c), 128)
    row = own[64:72]
    for i in range(8):
        sms[0, i : i + 1] = row[0:1, 128 * i : 128 * i + 128]
    sms[0, 8:24] = jnp.zeros((16, 128), F32)
    for i in (0, 1):
        rolled[i] = jnp.broadcast_to(row[i + 1 : i + 2, 0:128], (8, 128))
        sms[0, pl.ds(8 + 8 * i + z, 1)] = pltpu.roll(rolled[i], spread, 1)[0:1]

    barrier = pltpu.get_barrier_semaphore()
    peers = [{"dp_0": zo(k)} for k in (1, -1, 2, -2)]
    peers += [{"dp_1": yo(dy), "dp_2": lax.rem(c + dc, NC)} for dy in range(NY) for dc in range(NC) if dy or dc]
    peers += [{"tp": lax.rem(x + k, NX)} for k in range(1, NX)]
    for dev in peers:
        pl.semaphore_signal(barrier, inc=1, device_id=dev, device_id_type=MESH)
    pl.semaphore_wait(barrier, len(peers))

    pltpu.make_async_copy(pd_in, pd, loc.at[0]).wait()
    pltpu.make_async_copy(pu_in, pu, loc.at[1]).wait()

    def pair_d(*ks):
        for k in ks:
            started(
                pd.at[o, :, col(zo(k))], pr_d.at[zo(k)], s0_send.at[0], s0d_recv.at[zorder.index(k)], dp_2=o
            )

    def pair_u(*ks):
        for k in ks:
            started(
                pu.at[:, yo(k), o], pr_u.at[:, yo(k)], s0_send.at[1], s0u_recv.at[yorder.index(k)], dp_2=o
            )

    pair_d(4)
    pair_u(2)
    pair_d(3, -3)
    pair_u(1, -1)

    have = set()

    def need_d(k):
        if ("d", k) not in have:
            have.add(("d", k))
            i = zorder.index(k)
            arrived(pr_d.at[zo(k)], s0d_recv.at[i])

    def need_u(k):
        if ("u", k) not in have:
            have.add(("u", k))
            i = yorder.index(k)
            arrived(pr_u.at[:, yo(k)], s0u_recv.at[i])

    zslots, yslots = slots_of(NZ), slots_of(NY)

    def half_of(direction, h):
        return h if direction == 0 else 1 - h

    def sign(direction):
        return 1 if direction == 0 else -1

    def d_slot(direction, i):
        k, h = zslots[i]
        k = k * sign(direction)
        kk = 4 if k == -4 else k
        need_d(kk)
        rows = pl.ds(half_of(direction, h) * 256, 256)
        val = pd[c, rows, col(zo(kk))].astype(F32) + pr_d[zo(kk), rows].astype(F32)
        if i >= 2:
            arrived(dr.at[direction, i - 2], d_recv.at[direction, i - 2])
            val = val + dr[direction, i - 2]
        ds[direction, i] = val
        started(
            ds.at[direction, i], dr.at[direction, i], d_send.at[direction], d_recv.at[direction, i],
            dp_0=zo(sign(direction)),
        )

    def u_slot(direction, i):
        k, h = yslots[i]
        k = k * sign(direction)
        kk = 2 if k == -2 else k
        need_u(kk)
        part = pl.ds(half_of(direction, h) * 4, 4)
        val = pu[part, yo(kk), c].astype(F32) + pr_u[part, yo(kk)].astype(F32)
        if i >= 2:
            arrived(ur.at[direction, i - 2], u_recv.at[direction, i - 2])
            val = val + ur[direction, i - 2]
        us[direction, i] = val
        started(
            us.at[direction, i], ur.at[direction, i], u_send.at[direction], u_recv.at[direction, i],
            dp_1=yo(sign(direction)),
        )

    def z_slot(direction, i):
        k, h = zslots[i]
        k = k * sign(direction)
        rows = pl.ds(half_of(direction, h) * 8, 8)
        val = sum_u[zo(k), rows]
        if i >= 2:
            arrived(zr.at[direction, i - 2], z_recv.at[direction, i - 2])
            val = val + zr[direction, i - 2]
        zs[direction, i] = val
        started(
            zs.at[direction, i], zr.at[direction, i], z_send.at[direction], z_recv.at[direction, i],
            dp_0=zo(sign(direction)),
        )

    for i in (0, 1):
        for direction in (0, 1):
            d_slot(direction, i)
        for direction in (0, 1):
            u_slot(direction, i)

    pair_d(2, -2, 1, -1)
    started(sms.at[0], smr.at[0], sm_send.at[0], sm_recv.at[0], dp_2=o)
    pair_d(0)
    pair_u(0)
    for i in (2, 3):
        for direction in (0, 1):
            d_slot(direction, i)
    for direction in (0, 1):
        u_slot(direction, 2)

    arrived(smr.at[0], sm_recv.at[0])
    sms[1] = sms[0] + smr[0]
    for dy in range(1, NY):
        started(sms.at[1], smr.at[dy], sm_send.at[1], sm_recv.at[dy], dp_1=yo(dy))

    def norm_on(k):
        for direction in (0, 1):
            if 0 < k <= 4 - direction:
                arrived(smr.at[3 + 4 * direction + k], sm_recv.at[3 + 4 * direction + k])
            if k < 4 - direction:
                src = smr.at[3 + 4 * direction + k] if k else sms.at[2]
                i = 4 + 4 * direction + k
                started(src, smr.at[i], sm_send.at[2 + direction], sm_recv.at[i], dp_0=zo(sign(direction)))

    for i in (4, 5, 6):
        for direction in (0, 1):
            d_slot(direction, i)

    need_u(0)
    for h in (0, 1):
        part = pl.ds(4 * h, 4)
        val = pu[part, y, c].astype(F32) + pr_u[part, y].astype(F32)
        for direction in (0, 1):
            i = 2 if half_of(direction, 0) == h else 1
            arrived(ur.at[direction, i], u_recv.at[direction, i])
            val = val + ur[direction, i]
        sum_u[part] = val
    for i in (0, 1):
        for direction in (0, 1):
            z_slot(direction, i)

    total = sms[1]
    for dy in range(1, NY):
        arrived(smr.at[dy], sm_recv.at[dy])
        total = total + smr[dy]
    sms[2] = total
    norm_on(0)

    need_d(0)
    for h in (0, 1):
        rows = pl.ds(256 * h, 256)
        val = pd[c, rows, col(z)].astype(F32) + pr_d[z, rows].astype(F32)
        for direction in (0, 1):
            i = 6 if half_of(direction, 0) == h else 5
            arrived(dr.at[direction, i], d_recv.at[direction, i])
            val = val + dr[direction, i]
        for b in (0, 1):
            gs[:, :, pl.ds(256 * h + 128 * b, 128)] = val[128 * b : 128 * b + 128].T.reshape(NY * NC, 16, 128)
    for dy in range(NY):
        for dc in range(NC):
            if dy or dc:
                yt, ct = yo(dy), lax.rem(c + dc, NC)
                started(
                    gs.at[yt * NC + ct], gr.at[c, dy], g_send.at[0], g_recv.at[dy, dc], dp_1=yt, dp_2=ct
                )
    gr[c, 0] = gs[y * NC + c]

    def z_step(*steps):
        for i in steps:
            for direction in (0, 1):
                z_slot(direction, i)

    lane = lax.broadcasted_iota(jnp.int32, (16, 128), 1)

    def tp_send(which, mean, master):
        own = jnp.sum(master * master, axis=1, keepdims=True)
        slope = jnp.sum(mean * mean, axis=1, keepdims=True)
        tps[which] = jnp.where(lane < 64, own, slope)
        for k in range(1, NX):
            started(
                tps.at[which], tpr.at[which, k - 1], t_send.at[which], t_recv.at[which, k - 1],
                tp=lax.rem(x + k, NX),
            )

    def tp_total(which):
        val = tps[which]
        for k in range(1, NX):
            arrived(tpr.at[which, k - 1], t_recv.at[which, k - 1])
            val = val + tpr[which, k - 1]
        return jnp.sqrt(val[:, 0:1]) * lax.rsqrt(val[:, 64:65] + 1e-06)

    def down_sum():
        for dy in range(NY):
            for dc in range(NC):
                if dy or dc:
                    cs = lax.rem(c + dc, NC)
                    arrived(gr.at[cs, dy], g_recv.at[dy, dc])
        for h in (0, 1):
            sd[:, pl.ds(512 * h, 512)] = (gr[h, 0] + gr[h, 1] + gr[h, 2] + gr[h, 3]) * 0.125
        tp_send(1, sd[...], md[...])

    def up_sum():
        for h in (0, 1):
            rows = pl.ds(8 * h, 8)
            val = sum_u[z, rows]
            for direction in (0, 1):
                i = 6 if half_of(direction, 0) == h else 5
                arrived(zr.at[direction, i], z_recv.at[direction, i])
                val = val + zr[direction, i]
            su[rows] = val * 0.125
        tp_send(0, su[...], mu[...])

    def down_update():
        stepped, state = updated(md[...], vd[...], sd[...] * tp_total(1))
        state_out[16:32] = stepped
        state_out[48:64] = state
        turned = stepped.astype(BF16)
        gds[0] = turned[:, :512]
        gds[1] = turned[:, 512:]
        for dy in range(NY):
            for dc in range(NC):
                if dy or dc:
                    yt, ct = yo(dy), lax.rem(c + dc, NC)
                    started(gds.at[ct], gd.at[y, c], gd_send.at[0], gd_recv.at[dy, dc], dp_1=yt, dp_2=ct)
        gd[y, c] = gds[c]

    def up_update():
        stepped, state = updated(mu[...], vu[...], su[...] * tp_total(0))
        state_out[0:16] = stepped
        state_out[32:48] = state
        out_u[z, y, c] = stepped.astype(BF16)

    def norm_update():
        total = sms[2]
        for k in range(7):
            total = total + smr[4 + k]
        stepped, state = updated(total[8:16], total[16:24], total[0:8] * 0.125)
        rolled[0] = stepped
        rolled[1] = state
        for i in range(8):
            nout[0:1, 128 * i : 128 * i + 128] = stepped[i : i + 1]
        back = lax.rem(128 - spread, 128)
        for i in (0, 1):
            mine = jnp.broadcast_to(rolled[i, pl.ds(z, 1)], (8, 128))
            nout[8 + 8 * i : 16 + 8 * i, 0:128] = pltpu.roll(mine, back, 1)

    lanes = lambda h: pl.ds(512 * h, 512)

    def to_partner_u(zt, yt):
        piece = out_u.at[zt, yt, c]
        started(piece, piece, pair_send.at[0], pair_recv.at[0], dp_2=o)

    def to_y(kz):
        for direction in (0, 1):
            piece = out_u.at[zo(kz), y, c]
            started(
                piece, piece, agy_send.at[direction], agy_recv.at[direction, 0, kz % NZ], dp_1=yo(sign(direction))
            )
        to_partner_u(zo(kz), y)

    def to_z(direction, k):
        s = sign(direction)
        piece = out_u.at[zo(-s * k), y, c]
        started(piece, piece, agz_send.at[direction], agz_recv.at[direction, k], dp_0=zo(s))
        if k:
            piece = piece.at[:, lanes(half_of(direction, 0))]
        started(piece, piece, agz_send.at[direction], agz_recv.at[direction, k + 1], dp_0=zo(2 * s))

    def z_came(direction, k):
        piece = out_u.at[zo(-sign(direction) * k), y, c]
        if k == 4:
            piece = piece.at[:, lanes(half_of(direction, 0))]
        arrived(piece, agz_recv.at[direction, k - 1])

    def y_came(kz):
        for direction in (0, 1):
            s = sign(direction)
            piece = out_u.at[zo(kz), yo(-s), c]
            arrived(piece, agy_recv.at[direction, 0, kz % NZ])
            half = piece.at[:, lanes(direction)]
            started(half, half, agy_send.at[direction], agy_recv.at[direction, 1, kz % NZ], dp_1=yo(s))
            to_partner_u(zo(kz), yo(-s))

    def y_far(kz):
        for direction in (0, 1):
            half = out_u.at[zo(kz), yo(2), c].at[:, lanes(direction)]
            arrived(half, agy_recv.at[direction, 1, kz % NZ])
        to_partner_u(zo(kz), yo(2))

    def d_block(kz, h):
        return out_d.at[pl.ds(pl.multiple_of(c * 512 + h * 256, 256), 256), col(zo(kz))]

    def to_dz(direction, k, h):
        block = d_block(-sign(direction) * k, h)
        started(block, block, agd_send.at[direction], agd_recv.at[direction, k, h], dp_0=zo(sign(direction)))

    def to_partner_d(kz, h):
        block = d_block(kz, h)
        started(block, block, pair_send.at[1], pair_recv.at[1], dp_2=o)

    def turn():
        for dy in range(NY):
            for dc in range(NC):
                if dy or dc:
                    arrived(gd.at[yo(-dy), lax.rem(c + dc, NC)], gd_recv.at[dy, dc])
        for b in range(4):
            block = gd[:, :, :, 128 * b : 128 * b + 128].reshape(128, 128).astype(F32)
            out_d[pl.ds(pl.multiple_of(c * 512 + b * 128, 128), 128), col(z)] = block.T.astype(BF16)
        for h in (0, 1):
            for direction in (0, 1):
                to_dz(direction, 0, half_of(direction, h))
        for h in (0, 1):
            to_partner_d(0, h)

    def d_came(k, h):
        for direction in (0, 1):
            hh = half_of(direction, h)
            if k == 4 and h == 1:
                continue
            arrived(d_block(-sign(direction) * k, hh), agd_recv.at[direction, k - 1, hh])
            if k < 3 or (k == 3 and h == 0):
                to_dz(direction, k, hh)
            to_partner_d(-sign(direction) * k, hh)

    def first_u():
        for direction in (0, 1):
            to_z(direction, 0)
        to_y(0)

    def u_came(k):
        for direction in (0, 1):
            z_came(direction, k)
            if k == 2:
                to_z(direction, k)
        if k < 4:
            for direction in (0, 1):
                to_y(-sign(direction) * k)
        else:
            to_y(4)

    z_step(2, 3)
    norm_on(1)
    down_sum()
    z_step(4)
    down_update()
    z_step(5, 6)
    turn()
    up_sum()
    norm_on(2)
    d_came(1, 0)
    up_update()
    first_u()
    d_came(1, 1)
    d_came(2, 0)
    y_came(0)
    u_came(1)
    norm_on(3)
    d_came(2, 1)
    u_came(2)
    y_far(0)
    for kz in (-1, 1):
        y_came(kz)
    d_came(3, 0)
    d_came(3, 1)
    norm_on(4)
    norm_update()
    u_came(3)
    for kz in (-1, 1):
        y_far(kz)
    for kz in (-2, 2):
        y_came(kz)
    d_came(4, 0)
    u_came(4)
    for kz in (-2, 2):
        y_far(kz)
    for kz in (-3, 3):
        y_came(kz)
    y_came(4)
    for kz in (-3, 3):
        y_far(kz)
    y_far(4)

    arrived(out_u.at[:, :, o], pair_recv.at[0])
    arrived(out_d.at[pl.ds(pl.multiple_of(o * 512, 512), 512)], pair_recv.at[1])

    def left(ref, sem):
        pltpu.make_async_copy(ref, ref, sem).wait()

    left(pr_d, s0_send.at[0])
    left(pr_u, s0_send.at[1])
    left(smr.at[0], sm_send.at[0])
    left(smr.at[pl.ds(0, 3)], sm_send.at[1])
    left(smr.at[pl.ds(0, 4)], sm_send.at[2])
    left(smr.at[pl.ds(0, 3)], sm_send.at[3])
    left(gs.at[pl.ds(0, 7)], g_send.at[0])
    left(pr_d.at[0, pl.ds(0, 448)], gd_send.at[0])
    left(out_u.at[:, :, c], pair_send.at[0])
    left(out_d.at[pl.ds(pl.multiple_of(c * 512, 512), 512)], pair_send.at[1])
    for direction in (0, 1):
        left(ds.at[direction], d_send.at[direction])
        left(us.at[direction], u_send.at[direction])
        left(zs.at[direction], z_send.at[direction])
        left(tpr.at[direction], t_send.at[direction])
        left(pr_d.at[0, pl.ds(0, 448)], agz_send.at[direction])
        left(pr_d.at[pl.ds(0, 3)], agy_send.at[direction])
        left(pr_d.at[pl.ds(0, 7), pl.ds(0, 256)], agd_send.at[direction])


def finish(cu, cd, st, cu_out, cd_out, su, sd, qu, qd, sem):
    copies = [pltpu.make_async_copy(cu, cu_out, sem.at[0]), pltpu.make_async_copy(cd, cd_out, sem.at[1])]
    for i, ref in enumerate((su, sd, qu, qd)):
        copies.append(pltpu.make_async_copy(st.at[pl.ds(16 * i, 16)], ref, sem.at[2 + i]))
    for copy in copies:
        copy.start()
    for copy in copies:
        copy.wait()


def local(pu, pd, pn, mu, md, mn, vu, vd, vn):
    vm = pl.BlockSpec(memory_space=pltpu.VMEM)
    hbm = pl.BlockSpec(memory_space=pl.ANY)
    sds = jax.ShapeDtypeStruct
    dma = pltpu.SemaphoreType.DMA
    wide = lambda v: jnp.pad(v.reshape(1, 16), ((0, 0), (0, 1008)))
    own = jnp.concatenate([mu, md.T, vu, vd.T, pn.astype(F32), wide(mn), wide(vn), jnp.zeros((5, 1024), F32)], axis=0)
    up, down, state = sds((NZ, NY, NC, 16, 1024), BF16), sds((1024, 1024), BF16), sds((16, 1024), F32)
    out_u, out_d, states, nout = pl.pallas_call(
        kernel,
        out_shape=(up, down, sds((64, 1024), F32), sds((24, 1024), F32)),
        in_specs=[vm, hbm, hbm],
        out_specs=(vm,) * 4,
        scratch_shapes=[
            pltpu.VMEM((NZ, NY, NC, 16, 1024), BF16),
            pltpu.VMEM((2, 512, 1024), BF16),
            pltpu.VMEM((NZ, NY, 16, 1024), BF16),
            pltpu.VMEM((NZ, 512, 128), BF16),
            pltpu.VMEM((2, 7, 256, 128), F32),
            pltpu.VMEM((2, 7, 256, 128), F32),
            pltpu.VMEM((2, 3, 4, 16, 1024), F32),
            pltpu.VMEM((2, 3, 4, 16, 1024), F32),
            pltpu.VMEM((NZ, 16, 1024), F32),
            pltpu.VMEM((2, 7, 8, 1024), F32),
            pltpu.VMEM((2, 7, 8, 1024), F32),
            pltpu.VMEM((8, 16, 512), F32),
            pltpu.VMEM((2, 4, 16, 512), F32),
            pltpu.VMEM((2, 16, 128), F32),
            pltpu.VMEM((2, 3, 16, 128), F32),
            pltpu.VMEM((2, 16, 512), BF16),
            pltpu.VMEM((4, 2, 16, 512), BF16),
            pltpu.VMEM((3, 24, 128), F32),
            pltpu.VMEM((11, 24, 128), F32),
            pltpu.VMEM((2, 8, 128), F32),
            pltpu.VMEM((16, 1024), F32),
            pltpu.VMEM((16, 1024), F32),
            dma((2,)), dma((2,)), dma((4,)), dma((8,)),
            dma((2,)), dma((2, 7)), dma((2,)), dma((2, 3)), dma((2,)), dma((2, 7)),
            dma((1,)), dma((4, 2)), dma((2,)), dma((2, 3)), dma((4,)), dma((11,)),
            dma((2,)), dma((2, 4)), dma((2,)), dma((2, 2, 8)), dma((2,)), dma((2, 4, 2)),
            dma((1,)), dma((4, 2)), dma((2,)), dma((2,)),
        ],
        compiler_params=pltpu.CompilerParams(
            collective_id=0, has_side_effects=True, vmem_limit_bytes=VMEM_LIMIT
        ),
        name="update",
    )(own, pu.reshape(NZ, NY, NC, 16, 1024), pd.reshape(2, 512, 1024))
    cu, cd, su, sd, qu, qd = pl.pallas_call(
        finish,
        out_shape=(up, down, state, state, state, state),
        in_specs=[vm] * 3,
        out_specs=(hbm,) * 6,
        scratch_shapes=[dma((6,))],
        compiler_params=pltpu.CompilerParams(vmem_limit_bytes=2**20),
        name="finish",
    )(out_u, out_d, states)
    return (
        cu.reshape(1024, 1024), cd, nout[0].astype(BF16),
        su, sd.T, nout[8, :16], qu, qd.T, nout[16, :16],
    )


def solution(mesh):
    finer = Mesh(mesh.devices.reshape(NZ, NY, NC, mesh.shape["tp"]), (*DP, "tp"))
    return jax.shard_map(
        local,
        mesh=finer,
        in_specs=(
            P(DP, None, "tp"), P(DP, "tp", None), P(DP, None),
            P(DP, "tp"), P("tp", DP), P(DP),
            P(DP, "tp"), P("tp", DP), P(DP),
        ),
        out_specs=(
            P(None, "tp"), P("tp", None), P(),
            P(DP, "tp"), P("tp", DP), P(DP),
            P(DP, "tp"), P("tp", DP), P(DP),
        ),
        check_vma=False,
    )
```

```python
import functools

import jax
import jax.numpy as jnp
from jax import lax
from jax.experimental import pallas as pl
from jax.experimental.pallas import tpu as pltpu
from jax.sharding import Mesh
from jax.sharding import PartitionSpec as P

DP = ("dp_0", "dp_1", "dp_2")
NZ, NY, NC, NX = 8, 4, 2, 4
MESH = pl.DeviceIdType.MESH
F32, BF16 = jnp.float32, jnp.bfloat16

learn_rate = 0.025
hold_rate = 0.8

VMEM_LIMIT = 49 * 2**20


def updated(master, memory, mean):
    state = hold_rate * memory + (1.0 - hold_rate) * mean * mean
    return master - learn_rate * mean * lax.rsqrt(state + 1e-06), state


def slots_of(n):
    out = [(n // 2, 0)]
    for k in range(n // 2 - 1, 0, -1):
        out += [(k, 1), (k, 0)]
    return out


def kernel(
    own, pu_in, pd_in,
    out_u, out_d, state_out, nout,
    pu, pd, pr_u, pr_d, ds, dr, us, ur, sum_u, zs, zr, gs, gr, tps, tpr, gds, gd, sms, smr, rolled, su, sd,
    loc, s0_send, s0u_recv, s0d_recv, d_send, d_recv, u_send, u_recv, z_send, z_recv,
    g_send, g_recv, t_send, t_recv, sm_send, sm_recv,
    agz_send, agz_recv, agy_send, agy_recv, agd_send, agd_recv, gd_send, gd_recv, pair_send, pair_recv,
):
    z, y, c, x = (lax.axis_index(a) for a in ("dp_0", "dp_1", "dp_2", "tp"))
    o = 1 - c
    zo = lambda k: lax.rem(z + k + NZ, NZ)
    yo = lambda k: lax.rem(y + k + NY, NY)

    def rcopy(src, dst, ssem, rsem, **dev):
        cp = pltpu.make_async_remote_copy(
            src_ref=src, dst_ref=dst, send_sem=ssem, recv_sem=rsem, device_id=dev, device_id_type=MESH
        )
        return cp

    def started(*args, **dev):
        rcopy(*args, **dev).start()

    def arrived(dst, rsem):
        pltpu.make_async_copy(dst, dst, rsem).wait()

    zorder = (4, 3, -3, 2, -2, 1, -1, 0)
    yorder = (2, 1, -1, 0)
    col = lambda zt: pl.ds(pl.multiple_of(zt * 128, 128), 128)

    pltpu.make_async_copy(pd_in, pd, loc.at[0]).start()
    pltpu.make_async_copy(pu_in, pu, loc.at[1]).start()
    mu, md, vu, vd = (own.at[pl.ds(16 * i, 16)] for i in range(4))

    spread = lax.rem(16 * (y * NC + c), 128)
    row = own[64:72]
    for i in range(8):
        sms[0, i : i + 1] = row[0:1, 128 * i : 128 * i + 128]
    sms[0, 8:24] = jnp.zeros((16, 128), F32)
    for i in (0, 1):
        rolled[i] = jnp.broadcast_to(row[i + 1 : i + 2, 0:128], (8, 128))
        sms[0, pl.ds(8 + 8 * i + z, 1)] = pltpu.roll(rolled[i], spread, 1)[0:1]

    barrier = pltpu.get_barrier_semaphore()
    peers = [{"dp_0": zo(k)} for k in (1, -1, 2, -2)]
    peers += [{"dp_1": yo(dy), "dp_2": lax.rem(c + dc, NC)} for dy in range(NY) for dc in range(NC) if dy or dc]
    peers += [{"tp": lax.rem(x + k, NX)} for k in range(1, NX)]
    for dev in peers:
        pl.semaphore_signal(barrier, inc=1, device_id=dev, device_id_type=MESH)
    pl.semaphore_wait(barrier, len(peers))

    pltpu.make_async_copy(pd_in, pd, loc.at[0]).wait()
    pltpu.make_async_copy(pu_in, pu, loc.at[1]).wait()

    def pair_d(*ks):
        for k in ks:
            started(
                pd.at[o, :, col(zo(k))], pr_d.at[zo(k)], s0_send.at[0], s0d_recv.at[zorder.index(k)], dp_2=o
            )

    def pair_u(*ks):
        for k in ks:
            started(
                pu.at[:, yo(k), o], pr_u.at[:, yo(k)], s0_send.at[1], s0u_recv.at[yorder.index(k)], dp_2=o
            )

    pair_d(4)
    pair_u(2)
    pair_d(3, -3)
    pair_u(1, -1)

    have = set()

    def need_d(k):
        if ("d", k) not in have:
            have.add(("d", k))
            i = zorder.index(k)
            arrived(pr_d.at[zo(k)], s0d_recv.at[i])

    def need_u(k):
        if ("u", k) not in have:
            have.add(("u", k))
            i = yorder.index(k)
            arrived(pr_u.at[:, yo(k)], s0u_recv.at[i])

    zslots, yslots = slots_of(NZ), slots_of(NY)

    def half_of(direction, h):
        return h if direction == 0 else 1 - h

    def sign(direction):
        return 1 if direction == 0 else -1

    def d_slot(direction, i):
        k, h = zslots[i]
        k = k * sign(direction)
        kk = 4 if k == -4 else k
        need_d(kk)
        rows = pl.ds(half_of(direction, h) * 256, 256)
        val = pd[c, rows, col(zo(kk))].astype(F32) + pr_d[zo(kk), rows].astype(F32)
        if i >= 2:
            arrived(dr.at[direction, i - 2], d_recv.at[direction, i - 2])
            val = val + dr[direction, i - 2]
        ds[direction, i] = val
        started(
            ds.at[direction, i], dr.at[direction, i], d_send.at[direction], d_recv.at[direction, i],
            dp_0=zo(sign(direction)),
        )

    def u_slot(direction, i):
        k, h = yslots[i]
        k = k * sign(direction)
        kk = 2 if k == -2 else k
        need_u(kk)
        part = pl.ds(half_of(direction, h) * 4, 4)
        val = pu[part, yo(kk), c].astype(F32) + pr_u[part, yo(kk)].astype(F32)
        if i >= 2:
            arrived(ur.at[direction, i - 2], u_recv.at[direction, i - 2])
            val = val + ur[direction, i - 2]
        us[direction, i] = val
        started(
            us.at[direction, i], ur.at[direction, i], u_send.at[direction], u_recv.at[direction, i],
            dp_1=yo(sign(direction)),
        )

    def z_slot(direction, i):
        k, h = zslots[i]
        k = k * sign(direction)
        rows = pl.ds(half_of(direction, h) * 8, 8)
        val = sum_u[zo(k), rows]
        if i >= 2:
            arrived(zr.at[direction, i - 2], z_recv.at[direction, i - 2])
            val = val + zr[direction, i - 2]
        zs[direction, i] = val
        started(
            zs.at[direction, i], zr.at[direction, i], z_send.at[direction], z_recv.at[direction, i],
            dp_0=zo(sign(direction)),
        )

    for i in (0, 1):
        for direction in (0, 1):
            d_slot(direction, i)
        for direction in (0, 1):
            u_slot(direction, i)

    pair_d(2, -2, 1, -1)
    started(sms.at[0], smr.at[0], sm_send.at[0], sm_recv.at[0], dp_2=o)
    pair_d(0)
    pair_u(0)
    for i in (2, 3):
        for direction in (0, 1):
            d_slot(direction, i)
    for direction in (0, 1):
        u_slot(direction, 2)

    arrived(smr.at[0], sm_recv.at[0])
    sms[1] = sms[0] + smr[0]
    for dy in range(1, NY):
        started(sms.at[1], smr.at[dy], sm_send.at[1], sm_recv.at[dy], dp_1=yo(dy))

    def norm_on(k):
        for direction in (0, 1):
            if 0 < k <= 4 - direction:
                arrived(smr.at[3 + 4 * direction + k], sm_recv.at[3 + 4 * direction + k])
            if k < 4 - direction:
                src = smr.at[3 + 4 * direction + k] if k else sms.at[2]
                i = 4 + 4 * direction + k
                started(src, smr.at[i], sm_send.at[2 + direction], sm_recv.at[i], dp_0=zo(sign(direction)))

    for i in (4, 5, 6):
        for direction in (0, 1):
            d_slot(direction, i)

    need_u(0)
    for h in (0, 1):
        part = pl.ds(4 * h, 4)
        val = pu[part, y, c].astype(F32) + pr_u[part, y].astype(F32)
        for direction in (0, 1):
            i = 2 if half_of(direction, 0) == h else 1
            arrived(ur.at[direction, i], u_recv.at[direction, i])
            val = val + ur[direction, i]
        sum_u[part] = val
    for i in (0, 1):
        for direction in (0, 1):
            z_slot(direction, i)

    total = sms[1]
    for dy in range(1, NY):
        arrived(smr.at[dy], sm_recv.at[dy])
        total = total + smr[dy]
    sms[2] = total
    norm_on(0)

    need_d(0)
    for h in (0, 1):
        rows = pl.ds(256 * h, 256)
        val = pd[c, rows, col(z)].astype(F32) + pr_d[z, rows].astype(F32)
        for direction in (0, 1):
            i = 6 if half_of(direction, 0) == h else 5
            arrived(dr.at[direction, i], d_recv.at[direction, i])
            val = val + dr[direction, i]
        for b in (0, 1):
            gs[:, :, pl.ds(256 * h + 128 * b, 128)] = val[128 * b : 128 * b + 128].T.reshape(NY * NC, 16, 128)
    for dy in (2, 1, 3, 0):
        for dc in range(NC):
            if dy or dc:
                yt, ct = yo(dy), lax.rem(c + dc, NC)
                started(
                    gs.at[yt * NC + ct], gr.at[c, dy], g_send.at[0], g_recv.at[dy, dc], dp_1=yt, dp_2=ct
                )
    gr[c, 0] = gs[y * NC + c]

    def z_step(*steps):
        for i in steps:
            for direction in (0, 1):
                z_slot(direction, i)

    lane = lax.broadcasted_iota(jnp.int32, (16, 128), 1)

    def tp_send(which, mean, master):
        own = jnp.sum(master * master, axis=1, keepdims=True)
        slope = jnp.sum(mean * mean, axis=1, keepdims=True)
        tps[which] = jnp.where(lane < 64, own, slope)
        for k in range(1, NX):
            started(
                tps.at[which], tpr.at[which, k - 1], t_send.at[which], t_recv.at[which, k - 1],
                tp=lax.rem(x + k, NX),
            )

    def tp_total(which):
        val = tps[which]
        for k in range(1, NX):
            arrived(tpr.at[which, k - 1], t_recv.at[which, k - 1])
            val = val + tpr[which, k - 1]
        return jnp.sqrt(val[:, 0:1]) * lax.rsqrt(val[:, 64:65] + 1e-06)

    def down_sum():
        for dy in range(NY):
            for dc in range(NC):
                if dy or dc:
                    cs = lax.rem(c + dc, NC)
                    arrived(gr.at[cs, dy], g_recv.at[dy, dc])
        for h in (0, 1):
            sd[:, pl.ds(512 * h, 512)] = (gr[h, 0] + gr[h, 1] + gr[h, 2] + gr[h, 3]) * 0.125
        tp_send(1, sd[...], md[...])

    def up_sum():
        for h in (0, 1):
            rows = pl.ds(8 * h, 8)
            val = sum_u[z, rows]
            for direction in (0, 1):
                i = 6 if half_of(direction, 0) == h else 5
                arrived(zr.at[direction, i], z_recv.at[direction, i])
                val = val + zr[direction, i]
            su[rows] = val * 0.125
        tp_send(0, su[...], mu[...])

    def down_update():
        stepped, state = updated(md[...], vd[...], sd[...] * tp_total(1))
        state_out[16:32] = stepped
        state_out[48:64] = state
        turned = stepped.astype(BF16)
        gds[0] = turned[:, :512]
        gds[1] = turned[:, 512:]
        for dy in (2, 1, 3, 0):
            for dc in range(NC):
                if dy or dc:
                    yt, ct = yo(dy), lax.rem(c + dc, NC)
                    started(gds.at[ct], gd.at[y, c], gd_send.at[0], gd_recv.at[dy, dc], dp_1=yt, dp_2=ct)
        gd[y, c] = gds[c]

    def up_update():
        stepped, state = updated(mu[...], vu[...], su[...] * tp_total(0))
        state_out[0:16] = stepped
        state_out[32:48] = state
        out_u[z, y, c] = stepped.astype(BF16)

    def norm_update():
        total = sms[2]
        for k in range(7):
            total = total + smr[4 + k]
        stepped, state = updated(total[8:16], total[16:24], total[0:8] * 0.125)
        rolled[0] = stepped
        rolled[1] = state
        nout[0:8] = stepped
        back = lax.rem(128 - spread, 128)
        for i in (0, 1):
            mine = jnp.broadcast_to(rolled[i, pl.ds(z, 1)], (8, 128))
            nout[8 + 8 * i : 16 + 8 * i] = pltpu.roll(mine, back, 1)

    lanes = lambda h: pl.ds(512 * h, 512)

    def to_partner_u(zt, yt):
        piece = out_u.at[zt, yt, c]
        started(piece, piece, pair_send.at[0], pair_recv.at[0], dp_2=o)

    def to_y(kz):
        for direction in (0, 1):
            piece = out_u.at[zo(kz), y, c]
            started(
                piece, piece, agy_send.at[direction], agy_recv.at[direction, 0, kz % NZ], dp_1=yo(sign(direction))
            )
        to_partner_u(zo(kz), y)

    def to_z(direction, k):
        s = sign(direction)
        piece = out_u.at[zo(-s * k), y, c]
        started(piece, piece, agz_send.at[direction], agz_recv.at[direction, k], dp_0=zo(s))
        if k:
            piece = piece.at[:, lanes(half_of(direction, 0))]
        started(piece, piece, agz_send.at[direction], agz_recv.at[direction, k + 1], dp_0=zo(2 * s))

    def z_came(direction, k):
        piece = out_u.at[zo(-sign(direction) * k), y, c]
        if k == 4:
            piece = piece.at[:, lanes(half_of(direction, 0))]
        arrived(piece, agz_recv.at[direction, k - 1])

    def y_came(kz):
        for direction in (0, 1):
            s = sign(direction)
            piece = out_u.at[zo(kz), yo(-s), c]
            arrived(piece, agy_recv.at[direction, 0, kz % NZ])
            half = piece.at[:, lanes(direction)]
            started(half, half, agy_send.at[direction], agy_recv.at[direction, 1, kz % NZ], dp_1=yo(s))
            to_partner_u(zo(kz), yo(-s))

    def y_far(kz):
        for direction in (0, 1):
            half = out_u.at[zo(kz), yo(2), c].at[:, lanes(direction)]
            arrived(half, agy_recv.at[direction, 1, kz % NZ])
        to_partner_u(zo(kz), yo(2))

    def d_block(kz, h):
        return out_d.at[pl.ds(pl.multiple_of(c * 512 + h * 256, 256), 256), col(zo(kz))]

    def to_dz(direction, k, h):
        block = d_block(-sign(direction) * k, h)
        started(block, block, agd_send.at[direction], agd_recv.at[direction, k, h], dp_0=zo(sign(direction)))

    def to_partner_d(kz, h):
        block = d_block(kz, h)
        started(block, block, pair_send.at[1], pair_recv.at[1], dp_2=o)

    def turn():
        for dy in range(NY):
            for dc in range(NC):
                if dy or dc:
                    arrived(gd.at[yo(-dy), lax.rem(c + dc, NC)], gd_recv.at[dy, dc])
        for b in range(4):
            block = gd[:, :, :, 128 * b : 128 * b + 128].reshape(128, 128).astype(F32)
            out_d[pl.ds(pl.multiple_of(c * 512 + b * 128, 128), 128), col(z)] = block.T.astype(BF16)
        for direction in (0, 1):
            to_dz(direction, 0, half_of(direction, 0))

    def turn_rest():
        for direction in (0, 1):
            to_dz(direction, 0, half_of(direction, 1))
        for h in (0, 1):
            to_partner_d(0, h)

    def d_came(k, h):
        for direction in (0, 1):
            hh = half_of(direction, h)
            if k == 4 and h == 1:
                continue
            arrived(d_block(-sign(direction) * k, hh), agd_recv.at[direction, k - 1, hh])
            if k < 3 or (k == 3 and h == 0):
                to_dz(direction, k, hh)
            to_partner_d(-sign(direction) * k, hh)

    def first_u():
        for direction in (0, 1):
            to_z(direction, 0)
        to_y(0)

    def u_came(k):
        for direction in (0, 1):
            z_came(direction, k)
            if k == 2:
                to_z(direction, k)
        if k < 4:
            for direction in (0, 1):
                to_y(-sign(direction) * k)
        else:
            to_y(4)

    z_step(2, 3)
    norm_on(1)
    down_sum()
    z_step(4, 5, 6)
    down_update()
    up_sum()
    norm_on(2)
    turn()
    up_update()
    first_u()
    turn_rest()
    d_came(1, 0)
    y_came(0)
    u_came(1)
    norm_on(3)
    u_came(2)
    d_came(1, 1)
    y_far(0)
    d_came(2, 0)
    for kz in (-1, 1):
        y_came(kz)
    u_came(3)
    for kz in (-2, 2):
        y_came(kz)
    d_came(2, 1)
    u_came(4)
    for kz in (-1, 1):
        y_far(kz)
    norm_on(4)
    norm_update()
    d_came(3, 0)
    for kz in (-2, 2):
        y_far(kz)
    for kz in (-3, 3, 4):
        y_came(kz)
    d_came(3, 1)
    d_came(4, 0)
    for kz in (-3, 3, 4):
        y_far(kz)

    def pair_came():
        arrived(out_u.at[:, :, o], pair_recv.at[0])
        arrived(out_d.at[pl.ds(pl.multiple_of(o * 512, 512), 512)], pair_recv.at[1])

    pair_came()

    def left(ref, sem):
        pltpu.make_async_copy(ref, ref, sem).wait()

    left(pr_d, s0_send.at[0])
    left(pr_u, s0_send.at[1])
    left(smr.at[0], sm_send.at[0])
    left(smr.at[pl.ds(0, 3)], sm_send.at[1])
    left(smr.at[pl.ds(0, 4)], sm_send.at[2])
    left(smr.at[pl.ds(0, 3)], sm_send.at[3])
    left(gs.at[pl.ds(0, 7)], g_send.at[0])
    left(pr_d.at[0, pl.ds(0, 448)], gd_send.at[0])
    left(out_u.at[:, :, c], pair_send.at[0])
    left(out_d.at[pl.ds(pl.multiple_of(c * 512, 512), 512)], pair_send.at[1])
    for direction in (0, 1):
        left(ds.at[direction], d_send.at[direction])
        left(us.at[direction], u_send.at[direction])
        left(zs.at[direction], z_send.at[direction])
        left(tpr.at[direction], t_send.at[direction])
        left(pr_d.at[0, pl.ds(0, 448)], agz_send.at[direction])
        left(pr_d.at[pl.ds(0, 3)], agy_send.at[direction])
        left(pr_d.at[pl.ds(0, 7), pl.ds(0, 256)], agd_send.at[direction])


def finish(cu, cd, st, nout, cu_out, cd_out, su, sd, qu, qd, cn, sn, qn, sem):
    copies = [pltpu.make_async_copy(cu, cu_out, sem.at[0]), pltpu.make_async_copy(cd, cd_out, sem.at[1])]
    for i, ref in enumerate((su, sd, qu, qd)):
        copies.append(pltpu.make_async_copy(st.at[pl.ds(16 * i, 16)], ref, sem.at[2 + i]))
    for copy in copies:
        copy.start()
    cn[...] = nout[0:8].astype(BF16)
    sn[...] = nout[8:9, 0:16]
    qn[...] = nout[16:17, 0:16]
    for copy in copies:
        copy.wait()


def local(pu, pd, pn, mu, md, mn, vu, vd, vn):
    vm = pl.BlockSpec(memory_space=pltpu.VMEM)
    hbm = pl.BlockSpec(memory_space=pl.ANY)
    sds = jax.ShapeDtypeStruct
    dma = pltpu.SemaphoreType.DMA
    parts = (mu, md.T, vu, vd.T, pn.astype(F32), mn.reshape(1, 16), vn.reshape(1, 16))
    at = (0, 16, 32, 48, 64, 65, 66)
    own = sum(jnp.pad(v, ((i, 72 - i - v.shape[0]), (0, 1024 - v.shape[1]))) for i, v in zip(at, parts))
    up, down, state = sds((NZ, NY, NC, 16, 1024), BF16), sds((1024, 1024), BF16), sds((16, 1024), F32)
    out_u, out_d, states, nout = pl.pallas_call(
        kernel,
        out_shape=(up, down, sds((64, 1024), F32), sds((24, 128), F32)),
        in_specs=[vm, hbm, hbm],
        out_specs=(vm,) * 4,
        scratch_shapes=[
            pltpu.VMEM((NZ, NY, NC, 16, 1024), BF16),
            pltpu.VMEM((2, 512, 1024), BF16),
            pltpu.VMEM((NZ, NY, 16, 1024), BF16),
            pltpu.VMEM((NZ, 512, 128), BF16),
            pltpu.VMEM((2, 7, 256, 128), F32),
            pltpu.VMEM((2, 7, 256, 128), F32),
            pltpu.VMEM((2, 3, 4, 16, 1024), F32),
            pltpu.VMEM((2, 3, 4, 16, 1024), F32),
            pltpu.VMEM((NZ, 16, 1024), F32),
            pltpu.VMEM((2, 7, 8, 1024), F32),
            pltpu.VMEM((2, 7, 8, 1024), F32),
            pltpu.VMEM((8, 16, 512), F32),
            pltpu.VMEM((2, 4, 16, 512), F32),
            pltpu.VMEM((2, 16, 128), F32),
            pltpu.VMEM((2, 3, 16, 128), F32),
            pltpu.VMEM((2, 16, 512), BF16),
            pltpu.VMEM((4, 2, 16, 512), BF16),
            pltpu.VMEM((3, 24, 128), F32),
            pltpu.VMEM((11, 24, 128), F32),
            pltpu.VMEM((2, 8, 128), F32),
            pltpu.VMEM((16, 1024), F32),
            pltpu.VMEM((16, 1024), F32),
            dma((2,)), dma((2,)), dma((4,)), dma((8,)),
            dma((2,)), dma((2, 7)), dma((2,)), dma((2, 3)), dma((2,)), dma((2, 7)),
            dma((1,)), dma((4, 2)), dma((2,)), dma((2, 3)), dma((4,)), dma((11,)),
            dma((2,)), dma((2, 4)), dma((2,)), dma((2, 2, 8)), dma((2,)), dma((2, 4, 2)),
            dma((1,)), dma((4, 2)), dma((2,)), dma((2,)),
        ],
        compiler_params=pltpu.CompilerParams(
            collective_id=0, has_side_effects=True, vmem_limit_bytes=VMEM_LIMIT
        ),
        name="update",
    )(own, pu.reshape(NZ, NY, NC, 16, 1024), pd.reshape(2, 512, 1024))
    cu, cd, su, sd, qu, qd, cn, sn, qn = pl.pallas_call(
        finish,
        out_shape=(up, down, state, state, state, state, sds((8, 128), BF16), sds((1, 16), F32), sds((1, 16), F32)),
        in_specs=[vm] * 4,
        out_specs=(hbm,) * 6 + (vm,) * 3,
        scratch_shapes=[dma((6,))],
        compiler_params=pltpu.CompilerParams(vmem_limit_bytes=2**20),
        name="finish",
    )(out_u, out_d, states, nout)
    return (
        cu.reshape(1024, 1024), cd, cn.reshape(1024), su, sd.T, sn.reshape(16), qu, qd.T, qn.reshape(16),
    )


def solution(mesh):
    finer = Mesh(mesh.devices.reshape(NZ, NY, NC, mesh.shape["tp"]), (*DP, "tp"))
    return jax.shard_map(
        local,
        mesh=finer,
        in_specs=(
            P(DP, None, "tp"), P(DP, "tp", None), P(DP, None),
            P(DP, "tp"), P("tp", DP), P(DP),
            P(DP, "tp"), P("tp", DP), P(DP),
        ),
        out_specs=(
            P(None, "tp"), P("tp", None), P(),
            P(DP, "tp"), P("tp", DP), P(DP),
            P(DP, "tp"), P("tp", DP), P(DP),
        ),
        check_vma=False,
    )
```

```python
import functools

import jax
import jax.numpy as jnp
from jax import lax
from jax.experimental import pallas as pl
from jax.experimental.pallas import tpu as pltpu
from jax.sharding import Mesh
from jax.sharding import PartitionSpec as P

DP = ("dp_0", "dp_1", "dp_2")
NZ, NY, NC, NX = 8, 4, 2, 4
MESH = pl.DeviceIdType.MESH
F32, BF16 = jnp.float32, jnp.bfloat16

learn_rate = 0.025
hold_rate = 0.8

VMEM_LIMIT = 49 * 2**20


def updated(master, memory, mean):
    state = hold_rate * memory + (1.0 - hold_rate) * mean * mean
    return master - learn_rate * mean * lax.rsqrt(state + 1e-06), state


def slots_of(n):
    out = [(n // 2, 0)]
    for k in range(n // 2 - 1, 0, -1):
        out += [(k, 1), (k, 0)]
    return out


def kernel(
    own, pu_in, pd_in,
    out_u, out_d, state_out, nout,
    pu, pd, pr_u, pr_d, ds, dr, us, ur, sum_u, zs, zr, gs, gr, tps, tpr, gds, gd, sms, smr, rolled, su, sd,
    loc, s0_send, s0u_recv, s0d_recv, d_send, d_recv, u_send, u_recv, z_send, z_recv,
    g_send, g_recv, t_send, t_recv, sm_send, sm_recv,
    agz_send, agz_recv, agy_send, agy_recv, agd_send, agd_recv, gd_send, gd_recv, pair_send, pair_recv,
):
    z, y, c, x = (lax.axis_index(a) for a in ("dp_0", "dp_1", "dp_2", "tp"))
    o = 1 - c
    zo = lambda k: lax.rem(z + k + NZ, NZ)
    yo = lambda k: lax.rem(y + k + NY, NY)

    def rcopy(src, dst, ssem, rsem, **dev):
        cp = pltpu.make_async_remote_copy(
            src_ref=src, dst_ref=dst, send_sem=ssem, recv_sem=rsem, device_id=dev, device_id_type=MESH
        )
        return cp

    def started(*args, **dev):
        rcopy(*args, **dev).start()

    def arrived(dst, rsem):
        pltpu.make_async_copy(dst, dst, rsem).wait()

    zorder = (4, 3, -3, 2, -2, 1, -1, 0)
    yorder = (2, 1, -1, 0)
    col = lambda zt: pl.ds(pl.multiple_of(zt * 128, 128), 128)

    pltpu.make_async_copy(pd_in, pd, loc.at[0]).start()
    pltpu.make_async_copy(pu_in, pu, loc.at[1]).start()
    mu, md, vu, vd = (own.at[pl.ds(16 * i, 16)] for i in range(4))

    spread = lax.rem(16 * (y * NC + c), 128)
    row = own[64:72]
    for i in range(8):
        sms[0, i : i + 1] = row[0:1, 128 * i : 128 * i + 128]
    sms[0, 8:24] = jnp.zeros((16, 128), F32)
    for i in (0, 1):
        rolled[i] = jnp.broadcast_to(row[i + 1 : i + 2, 0:128], (8, 128))
        sms[0, pl.ds(8 + 8 * i + z, 1)] = pltpu.roll(rolled[i], spread, 1)[0:1]

    barrier = pltpu.get_barrier_semaphore()
    peers = [{"dp_0": zo(k)} for k in (1, -1, 2, -2)]
    peers += [{"dp_1": yo(dy), "dp_2": lax.rem(c + dc, NC)} for dy in range(NY) for dc in range(NC) if dy or dc]
    peers += [{"tp": lax.rem(x + k, NX)} for k in range(1, NX)]
    for dev in peers:
        pl.semaphore_signal(barrier, inc=1, device_id=dev, device_id_type=MESH)
    pl.semaphore_wait(barrier, len(peers))

    pltpu.make_async_copy(pd_in, pd, loc.at[0]).wait()
    pltpu.make_async_copy(pu_in, pu, loc.at[1]).wait()

    def pair_d(*ks):
        for k in ks:
            started(
                pd.at[o, :, col(zo(k))], pr_d.at[zo(k)], s0_send.at[0], s0d_recv.at[zorder.index(k)], dp_2=o
            )

    def pair_u(*ks):
        for k in ks:
            started(
                pu.at[:, yo(k), o], pr_u.at[:, yo(k)], s0_send.at[1], s0u_recv.at[yorder.index(k)], dp_2=o
            )

    pair_d(4)
    pair_u(2)
    pair_d(3, -3)
    pair_u(1, -1)

    have = set()

    def need_d(k):
        if ("d", k) not in have:
            have.add(("d", k))
            i = zorder.index(k)
            arrived(pr_d.at[zo(k)], s0d_recv.at[i])

    def need_u(k):
        if ("u", k) not in have:
            have.add(("u", k))
            i = yorder.index(k)
            arrived(pr_u.at[:, yo(k)], s0u_recv.at[i])

    zslots, yslots = slots_of(NZ), slots_of(NY)

    def half_of(direction, h):
        return h if direction == 0 else 1 - h

    def sign(direction):
        return 1 if direction == 0 else -1

    def d_slot(direction, i):
        k, h = zslots[i]
        k = k * sign(direction)
        kk = 4 if k == -4 else k
        need_d(kk)
        rows = pl.ds(half_of(direction, h) * 256, 256)
        val = pd[c, rows, col(zo(kk))].astype(F32) + pr_d[zo(kk), rows].astype(F32)
        if i >= 2:
            arrived(dr.at[direction, i - 2], d_recv.at[direction, i - 2])
            val = val + dr[direction, i - 2]
        ds[direction, i] = val
        started(
            ds.at[direction, i], dr.at[direction, i], d_send.at[direction], d_recv.at[direction, i],
            dp_0=zo(sign(direction)),
        )

    def u_slot(p, i):
        for direction in (0, 1):
            k, h = yslots[i]
            k = k * sign(direction)
            kk = 2 if k == -2 else k
            need_u(kk)
            part = pl.ds(half_of(direction, h) * 4, 4)
            val = pu[part, yo(kk), c, p].astype(F32) + pr_u[part, yo(kk), p].astype(F32)
            if i >= 2:
                arrived(ur.at[p, direction, i - 2], u_recv.at[p, direction, i - 2])
                val = val + ur[p, direction, i - 2]
            us[p, direction, i] = val
            started(
                us.at[p, direction, i], ur.at[p, direction, i], u_send.at[direction], u_recv.at[p, direction, i],
                dp_1=yo(sign(direction)),
            )

    def z_slot(p, i):
        for direction in (0, 1):
            k, h = zslots[i]
            k = k * sign(direction)
            val = sum_u[p, zo(k), :, lanes(half_of(direction, h))]
            if i >= 2:
                arrived(zr.at[p, direction, i - 2], z_recv.at[p, direction, i - 2])
                val = val + zr[p, direction, i - 2]
            zs[p, direction, i] = val
            started(
                zs.at[p, direction, i], zr.at[p, direction, i], z_send.at[direction], z_recv.at[p, direction, i],
                dp_0=zo(sign(direction)),
            )

    lanes = lambda h: pl.ds(512 * h, 512)

    for i in (0, 1):
        for direction in (0, 1):
            d_slot(direction, i)
        u_slot(0, i)
    pair_d(2, -2, 1, -1)
    started(sms.at[0], smr.at[0], sm_send.at[0], sm_recv.at[0], dp_2=o)
    pair_u(0)
    pair_d(0)

    def d_step(i):
        for direction in (0, 1):
            d_slot(direction, i)

    def norm_pair():
        arrived(smr.at[0], sm_recv.at[0])
        sms[1] = sms[0] + smr[0]
        for dy in range(1, NY):
            started(sms.at[1], smr.at[dy], sm_send.at[1], sm_recv.at[dy], dp_1=yo(dy))

    def norm_y():
        total = sms[1]
        for dy in range(1, NY):
            arrived(smr.at[dy], sm_recv.at[dy])
            total = total + smr[dy]
        sms[2] = total
        norm_on(0)

    def norm_on(k):
        for direction in (0, 1):
            if 0 < k <= 4 - direction:
                arrived(smr.at[3 + 4 * direction + k], sm_recv.at[3 + 4 * direction + k])
            if k < 4 - direction:
                src = smr.at[3 + 4 * direction + k] if k else sms.at[2]
                i = 4 + 4 * direction + k
                started(src, smr.at[i], sm_send.at[2 + direction], sm_recv.at[i], dp_0=zo(sign(direction)))

    def u_final(p):
        need_u(0)
        for h in (0, 1):
            part = pl.ds(4 * h, 4)
            val = pu[part, y, c, p].astype(F32) + pr_u[part, y, p].astype(F32)
            for direction in (0, 1):
                i = 2 if half_of(direction, 0) == h else 1
                arrived(ur.at[p, direction, i], u_recv.at[p, direction, i])
                val = val + ur[p, direction, i]
            sum_u[p, part] = val
        z_slot(p, 0)
        z_slot(p, 1)

    def d_final():
        need_d(0)
        for h in (0, 1):
            rows = pl.ds(256 * h, 256)
            val = pd[c, rows, col(z)].astype(F32) + pr_d[z, rows].astype(F32)
            for direction in (0, 1):
                i = 6 if half_of(direction, 0) == h else 5
                arrived(dr.at[direction, i], d_recv.at[direction, i])
                val = val + dr[direction, i]
            for b in (0, 1):
                gs[:, :, pl.ds(256 * h + 128 * b, 128)] = val[128 * b : 128 * b + 128].T.reshape(NY * NC, 16, 128)
        for dy in (2, 1, 3, 0):
            for dc in range(NC):
                if dy or dc:
                    yt, ct = yo(dy), lax.rem(c + dc, NC)
                    started(
                        gs.at[yt * NC + ct], gr.at[c, dy], g_send.at[0], g_recv.at[dy, dc], dp_1=yt, dp_2=ct
                    )
        gr[c, 0] = gs[y * NC + c]


    def tp_send(which, mean, master):
        n = mean.shape[0]
        lane = lax.broadcasted_iota(jnp.int32, (n, 128), 1)
        own = jnp.sum(master * master, axis=1, keepdims=True)
        slope = jnp.sum(mean * mean, axis=1, keepdims=True)
        tps[which, 0:n] = jnp.where(lane < 64, own, slope)
        for k in range(1, NX):
            started(
                tps.at[which, pl.ds(0, n)], tpr.at[which, k - 1, pl.ds(0, n)], t_send.at[which],
                t_recv.at[which, k - 1], tp=lax.rem(x + k, NX),
            )

    def tp_total(which, n):
        val = tps[which, 0:n]
        for k in range(1, NX):
            arrived(tpr.at[which, k - 1, pl.ds(0, n)], t_recv.at[which, k - 1])
            val = val + tpr[which, k - 1, 0:n]
        return jnp.sqrt(val[:, 0:1]) * lax.rsqrt(val[:, 64:65] + 1e-06)

    def down_sum():
        for dy in range(NY):
            for dc in range(NC):
                if dy or dc:
                    cs = lax.rem(c + dc, NC)
                    arrived(gr.at[cs, dy], g_recv.at[dy, dc])
        for h in (0, 1):
            sd[:, pl.ds(512 * h, 512)] = (gr[h, 0] + gr[h, 1] + gr[h, 2] + gr[h, 3]) * 0.125
        tp_send(2, sd[...], md[...])

    def up_sum(p):
        for h in (0, 1):
            val = sum_u[p, z, :, lanes(h)]
            for direction in (0, 1):
                i = 6 if half_of(direction, 0) == h else 5
                arrived(zr.at[p, direction, i], z_recv.at[p, direction, i])
                val = val + zr[p, direction, i]
            su[p, :, lanes(h)] = val * 0.125
        tp_send(p, su[p], mu[8 * p : 8 * p + 8])

    def down_update():
        stepped, state = updated(md[...], vd[...], sd[...] * tp_total(2, 16))
        state_out[16:32] = stepped
        state_out[48:64] = state
        turned = stepped.astype(BF16)
        gds[0] = turned[:, :512]
        gds[1] = turned[:, 512:]
        for dy in (2, 1, 3, 0):
            for dc in range(NC):
                if dy or dc:
                    yt, ct = yo(dy), lax.rem(c + dc, NC)
                    started(gds.at[ct], gd.at[y, c], gd_send.at[0], gd_recv.at[dy, dc], dp_1=yt, dp_2=ct)
        gd[y, c] = gds[c]

    def up_update(p):
        rows = pl.ds(8 * p, 8)
        stepped, state = updated(mu[rows], vu[rows], su[p] * tp_total(p, 8))
        state_out[8 * p : 8 * p + 8] = stepped
        state_out[32 + 8 * p : 40 + 8 * p] = state
        out_u[z, y, c, p] = stepped.astype(BF16)
        first_u(p)

    def norm_update():
        total = sms[2]
        for k in range(7):
            total = total + smr[4 + k]
        stepped, state = updated(total[8:16], total[16:24], total[0:8] * 0.125)
        rolled[0] = stepped
        rolled[1] = state
        nout[0:8] = stepped
        back = lax.rem(128 - spread, 128)
        for i in (0, 1):
            mine = jnp.broadcast_to(rolled[i, pl.ds(z, 1)], (8, 128))
            nout[8 + 8 * i : 16 + 8 * i] = pltpu.roll(mine, back, 1)

    def to_partner_u(p, zt, yt):
        piece = out_u.at[zt, yt, c, p]
        started(piece, piece, pair_send.at[0], pair_recv.at[0], dp_2=o)

    def to_y(p, kz):
        for direction in (0, 1):
            piece = out_u.at[zo(kz), y, c, p]
            started(
                piece, piece, agy_send.at[direction], agy_recv.at[p, direction, 0, kz % NZ], dp_1=yo(sign(direction))
            )
        to_partner_u(p, zo(kz), y)

    def to_z(p, direction, k):
        s = sign(direction)
        piece = out_u.at[zo(-s * k), y, c, p]
        started(piece, piece, agz_send.at[direction], agz_recv.at[p, direction, k], dp_0=zo(s))
        if k:
            piece = piece.at[:, lanes(half_of(direction, 0))]
        started(piece, piece, agz_send.at[direction], agz_recv.at[p, direction, k + 1], dp_0=zo(2 * s))

    def z_came(p, direction, k):
        piece = out_u.at[zo(-sign(direction) * k), y, c, p]
        if k == 4:
            piece = piece.at[:, lanes(half_of(direction, 0))]
        arrived(piece, agz_recv.at[p, direction, k - 1])

    def y_came(p, kz):
        for direction in (0, 1):
            s = sign(direction)
            piece = out_u.at[zo(kz), yo(-s), c, p]
            arrived(piece, agy_recv.at[p, direction, 0, kz % NZ])
            half = piece.at[:, lanes(direction)]
            started(half, half, agy_send.at[direction], agy_recv.at[p, direction, 1, kz % NZ], dp_1=yo(s))
            to_partner_u(p, zo(kz), yo(-s))

    def y_far(p, kz):
        for direction in (0, 1):
            half = out_u.at[zo(kz), yo(2), c, p].at[:, lanes(direction)]
            arrived(half, agy_recv.at[p, direction, 1, kz % NZ])
        to_partner_u(p, zo(kz), yo(2))

    def d_block(kz, h):
        return out_d.at[pl.ds(pl.multiple_of(c * 512 + h * 256, 256), 256), col(zo(kz))]

    def to_dz(direction, k, h):
        block = d_block(-sign(direction) * k, h)
        started(block, block, agd_send.at[direction], agd_recv.at[direction, k, h], dp_0=zo(sign(direction)))

    def to_partner_d(kz, h):
        block = d_block(kz, h)
        started(block, block, pair_send.at[1], pair_recv.at[1], dp_2=o)

    def turn():
        for dy in range(NY):
            for dc in range(NC):
                if dy or dc:
                    arrived(gd.at[yo(-dy), lax.rem(c + dc, NC)], gd_recv.at[dy, dc])
        for b in range(4):
            block = gd[:, :, :, 128 * b : 128 * b + 128].reshape(128, 128).astype(F32)
            out_d[pl.ds(pl.multiple_of(c * 512 + b * 128, 128), 128), col(z)] = block.T.astype(BF16)
        for direction in (0, 1):
            to_dz(direction, 0, half_of(direction, 0))

    def turn_rest():
        for direction in (0, 1):
            to_dz(direction, 0, half_of(direction, 1))
        for h in (0, 1):
            to_partner_d(0, h)

    def d_came(k, h):
        for direction in (0, 1):
            hh = half_of(direction, h)
            if k == 4 and h == 1:
                continue
            arrived(d_block(-sign(direction) * k, hh), agd_recv.at[direction, k - 1, hh])
            if k < 3 or (k == 3 and h == 0):
                to_dz(direction, k, hh)
            to_partner_d(-sign(direction) * k, hh)

    def first_u(p):
        for direction in (0, 1):
            to_z(p, direction, 0)
        to_y(p, 0)

    def u_came(p, k):
        for direction in (0, 1):
            z_came(p, direction, k)
            if k == 2:
                to_z(p, direction, k)
        for kz in ((-k, k) if k < 4 else (4,)):
            to_y(p, kz)

    events = []

    def at(time, step, *args):
        events.append((time, len(events), step, args))

    for i, t in zip(range(2, 7), (5.2, 8.0, 10.8, 13.6, 16.4)):
        at(t, d_step, i)
    at(5.4, u_slot, 0, 2)
    at(5.5, u_slot, 1, 0)
    at(5.5, u_slot, 1, 1)
    at(5.6, norm_pair)
    at(10.9, u_final, 0)
    at(13.7, u_slot, 1, 2)
    at(14.5, z_slot, 0, 2)
    at(14.6, z_slot, 0, 3)
    at(18.5, z_slot, 0, 4)
    at(18.6, z_slot, 0, 5)
    at(19.2, u_final, 1)
    at(19.3, norm_y)
    at(22.0, z_slot, 0, 6)
    at(22.2, d_final)
    at(23.0, z_slot, 1, 2)
    at(23.1, z_slot, 1, 3)
    at(24.0, norm_on, 1)
    at(26.0, up_sum, 0)
    at(26.3, z_slot, 1, 4)
    at(26.4, z_slot, 1, 5)
    at(27.3, down_sum)
    at(29.0, up_update, 0)
    at(29.4, z_slot, 1, 6)
    at(30.0, norm_on, 2)
    at(30.5, down_update)
    at(32.2, up_sum, 1)
    at(34.5, turn)
    at(35.2, up_update, 1)
    at(35.3, turn_rest)
    at(36.5, norm_on, 3)
    at(41.0, norm_on, 4)
    at(41.1, norm_update)
    for p, t in ((0, 29.0), (1, 35.2)):
        at(t + 3.0, y_came, p, 0)
        at(t + 3.2, u_came, p, 1)
        at(t + 4.0, u_came, p, 2)
        at(t + 6.0, y_far, p, 0)
        at(t + 7.2, u_came, p, 3)
        at(t + 8.0, u_came, p, 4)
        for kz in (-1, 1):
            at(t + 6.0, y_came, p, kz)
            at(t + 9.0, y_far, p, kz)
        for kz in (-2, 2):
            at(t + 7.3, y_came, p, kz)
            at(t + 10.2, y_far, p, kz)
        for kz in (-3, 3, 4):
            at(t + 11.0, y_came, p, kz)
            at(t + 14.0, y_far, p, kz)
    for k, h, t in ((1, 0, 38.4), (1, 1, 40.0), (2, 0, 42.2), (2, 1, 43.8), (3, 0, 46.0), (3, 1, 47.4), (4, 0, 49.0)):
        at(t, d_came, k, h)
    for _, _, step, args in sorted(events, key=lambda e: e[:2]):
        step(*args)

    def pair_came():
        arrived(out_u.at[:, :, o], pair_recv.at[0])
        arrived(out_d.at[pl.ds(pl.multiple_of(o * 512, 512), 512)], pair_recv.at[1])

    pair_came()

    def left(ref, sem):
        pltpu.make_async_copy(ref, ref, sem).wait()

    left(pr_d, s0_send.at[0])
    left(pr_u, s0_send.at[1])
    left(smr.at[0], sm_send.at[0])
    left(smr.at[pl.ds(0, 3)], sm_send.at[1])
    left(smr.at[pl.ds(0, 4)], sm_send.at[2])
    left(smr.at[pl.ds(0, 3)], sm_send.at[3])
    left(gs.at[pl.ds(0, 7)], g_send.at[0])
    left(pr_d.at[0, pl.ds(0, 448)], gd_send.at[0])
    left(tpr.at[2], t_send.at[2])
    left(out_u.at[:, :, c], pair_send.at[0])
    left(out_d.at[pl.ds(pl.multiple_of(c * 512, 512), 512)], pair_send.at[1])
    for direction in (0, 1):
        left(ds.at[direction], d_send.at[direction])
        left(us.at[:, direction], u_send.at[direction])
        left(zs.at[:, direction], z_send.at[direction])
        left(tpr.at[direction, :, pl.ds(0, 8)], t_send.at[direction])
        left(pr_d.at[0, pl.ds(0, 448)], agz_send.at[direction])
        left(pr_d.at[pl.ds(0, 3)], agy_send.at[direction])
        left(pr_d.at[pl.ds(0, 7), pl.ds(0, 256)], agd_send.at[direction])


def finish(cu, cd, st, nout, cu_out, cd_out, su, sd, qu, qd, cn, sn, qn, sem):
    copies = [pltpu.make_async_copy(cu, cu_out, sem.at[0]), pltpu.make_async_copy(cd, cd_out, sem.at[1])]
    for i, ref in enumerate((su, sd, qu, qd)):
        copies.append(pltpu.make_async_copy(st.at[pl.ds(16 * i, 16)], ref, sem.at[2 + i]))
    for copy in copies:
        copy.start()
    cn[...] = nout[0:8].astype(BF16)
    sn[...] = nout[8:9, 0:16]
    qn[...] = nout[16:17, 0:16]
    for copy in copies:
        copy.wait()


def local(pu, pd, pn, mu, md, mn, vu, vd, vn):
    vm = pl.BlockSpec(memory_space=pltpu.VMEM)
    hbm = pl.BlockSpec(memory_space=pl.ANY)
    sds = jax.ShapeDtypeStruct
    dma = pltpu.SemaphoreType.DMA
    parts = (mu, md.T, vu, vd.T, pn.astype(F32), mn.reshape(1, 16), vn.reshape(1, 16))
    at = (0, 16, 32, 48, 64, 65, 66)
    own = sum(jnp.pad(v, ((i, 72 - i - v.shape[0]), (0, 1024 - v.shape[1]))) for i, v in zip(at, parts))
    up, down, state = sds((NZ, NY, NC, 2, 8, 1024), BF16), sds((1024, 1024), BF16), sds((16, 1024), F32)
    out_u, out_d, states, nout = pl.pallas_call(
        kernel,
        out_shape=(up, down, sds((64, 1024), F32), sds((24, 128), F32)),
        in_specs=[vm, hbm, hbm],
        out_specs=(vm,) * 4,
        scratch_shapes=[
            pltpu.VMEM((NZ, NY, NC, 2, 8, 1024), BF16),
            pltpu.VMEM((2, 512, 1024), BF16),
            pltpu.VMEM((NZ, NY, 2, 8, 1024), BF16),
            pltpu.VMEM((NZ, 512, 128), BF16),
            pltpu.VMEM((2, 7, 256, 128), F32),
            pltpu.VMEM((2, 7, 256, 128), F32),
            pltpu.VMEM((2, 2, 3, 4, 8, 1024), F32),
            pltpu.VMEM((2, 2, 3, 4, 8, 1024), F32),
            pltpu.VMEM((2, NZ, 8, 1024), F32),
            pltpu.VMEM((2, 2, 7, 8, 512), F32),
            pltpu.VMEM((2, 2, 7, 8, 512), F32),
            pltpu.VMEM((8, 16, 512), F32),
            pltpu.VMEM((2, 4, 16, 512), F32),
            pltpu.VMEM((3, 16, 128), F32),
            pltpu.VMEM((3, 3, 16, 128), F32),
            pltpu.VMEM((2, 16, 512), BF16),
            pltpu.VMEM((4, 2, 16, 512), BF16),
            pltpu.VMEM((3, 24, 128), F32),
            pltpu.VMEM((11, 24, 128), F32),
            pltpu.VMEM((2, 8, 128), F32),
            pltpu.VMEM((2, 8, 1024), F32),
            pltpu.VMEM((16, 1024), F32),
            dma((2,)), dma((2,)), dma((4,)), dma((8,)),
            dma((2,)), dma((2, 7)), dma((2,)), dma((2, 2, 3)), dma((2,)), dma((2, 2, 7)),
            dma((1,)), dma((4, 2)), dma((3,)), dma((3, 3)), dma((4,)), dma((11,)),
            dma((2,)), dma((2, 2, 4)), dma((2,)), dma((2, 2, 2, 8)), dma((2,)), dma((2, 4, 2)),
            dma((1,)), dma((4, 2)), dma((2,)), dma((2,)),
        ],
        compiler_params=pltpu.CompilerParams(
            collective_id=0, has_side_effects=True, vmem_limit_bytes=VMEM_LIMIT
        ),
        name="update",
    )(own, pu.reshape(NZ, NY, NC, 2, 8, 1024), pd.reshape(2, 512, 1024))
    cu, cd, su, sd, qu, qd, cn, sn, qn = pl.pallas_call(
        finish,
        out_shape=(up, down, state, state, state, state, sds((8, 128), BF16), sds((1, 16), F32), sds((1, 16), F32)),
        in_specs=[vm] * 4,
        out_specs=(hbm,) * 6 + (vm,) * 3,
        scratch_shapes=[dma((6,))],
        compiler_params=pltpu.CompilerParams(vmem_limit_bytes=2**20),
        name="finish",
    )(out_u, out_d, states, nout)
    return (
        cu.reshape(1024, 1024), cd, cn.reshape(1024), su, sd.T, sn.reshape(16), qu, qd.T, qn.reshape(16),
    )


def solution(mesh):
    finer = Mesh(mesh.devices.reshape(NZ, NY, NC, mesh.shape["tp"]), (*DP, "tp"))
    return jax.shard_map(
        local,
        mesh=finer,
        in_specs=(
            P(DP, None, "tp"), P(DP, "tp", None), P(DP, None),
            P(DP, "tp"), P("tp", DP), P(DP),
            P(DP, "tp"), P("tp", DP), P(DP),
        ),
        out_specs=(
            P(None, "tp"), P("tp", None), P(),
            P(DP, "tp"), P("tp", DP), P(DP),
            P(DP, "tp"), P("tp", DP), P(DP),
        ),
        check_vma=False,
    )
```
